128 devices in a mesh: gx: 8 (over z_hi, y), gz: 16 (over z_lo, x, core).
Axes of the slice: x: 4, y: 4, z: 4 (z_hi: 2, z_lo: 2; z = z_hi * 2 + z_lo), core: 2. Of those that a mesh axis runs over, the one named last changes fastest.
Arguments:
- high_u: bfloat16 [256, 512, 512], P('gx', 'gz'), may hold values from -6 to 6
- high_v: bfloat16 [256, 512, 512], P('gx', 'gz'), may hold values from -6 to 6
- low_u: bfloat16 [2048, 512], P(('gx', 'gz')), may hold values from -0.25 to 0.25
- low_v: bfloat16 [2048, 512], P(('gx', 'gz')), may hold values from -0.25 to 0.25
- low_kx: int32 [2048], P(('gx', 'gz')), may hold values from 0 to 64, as said below
- low_kz: int32 [2048], P(('gx', 'gz')), may hold values from 0 to 64, as said below
- tau_inverse: bfloat16 [2048, 512, 512], P(('gx', 'gz')), may hold values from -0.25 to 0.25
Outputs:
- high_term: bfloat16 [256, 512, 512], P('gx', 'gz')
- low_response: float32 [2048, 512], P(('gx', 'gz'))
The draws below stay inside these ranges and needn't reach their ends.
Inputs may be any that keep to these rules, and one draw needn't show every extreme that they name: Slot m holds the retained mode (low_kx[m], low_kz[m]); no two slots hold the same pair; the device that holds slot m owns that mode. `low_kz`: paired with low_kx slot by slot.
All inputs are finite; a program needn't handle non-finite values.
Results may differ from the reference program's by a relative error of at most 0.0047.
Values may be sent and summed in bfloat16 or wider, within the bound.
No kernel may reach another device: no remote copies, remote signals or barrier semaphores. Data moves between devices by JAX's collectives and lax.ppermute only.
A program may use at most 128 MiB of HBM per device.

```python
import math
import jax
import jax.numpy as jnp
from jax import lax

NY = 512
KL = 32
LOW_DEV = 16
CX = 32
NX = 256
NZ = 512
LOW_MODES = 2048


def mode_pairs(key):
    side = 2 * KL + 1
    order = jax.random.permutation(jax.random.fold_in(key, 7), side * side)[:LOW_MODES]
    return ((order // side).astype(jnp.int32), (order % side).astype(jnp.int32))


def draw_low_kx(key, part):
    return mode_pairs(key)[0]


def draw_low_kz(key, part):
    return mode_pairs(key)[1]


def steps_of(own_key, dims, split, least, high):
    gain = 1.0
    for dim, parts in split:
        steps = jax.random.uniform(jax.random.fold_in(jax.random.fold_in(own_key, 6), dim), (parts,), jnp.float32, least / len(split), high / len(split))
        gain = gain * jnp.repeat(jnp.exp(steps), dims[dim] // parts).reshape((-1,) + (1,) * (len(dims) - 1 - dim))
    return gain


def centred(key, dims, deviation, bound, cuts=(), kind=jnp.bfloat16):
    entries = jax.random.normal(key, dims, jnp.float32) * deviation
    if len(cuts) > 0:
        entries = steps_of(key, dims, cuts, -0.22, 0.18) * entries
    return jnp.clip(entries, min=-bound, max=bound).astype(kind)


def setup_inputs(seed: int = 0) -> dict:
    seeds = jax.random.split(jax.random.key(seed), 8)
    return {
        "high_u": centred(seeds[0], (NX, NZ, NY), 1.0, 6.0, ((0, 8), (1, 16))),
        "high_v": centred(seeds[1], (NX, NZ, NY), 1.0, 6.0, ((0, 8), (1, 16))),
        "low_u": centred(seeds[2], (LOW_MODES, NY), (LOW_MODES // 4) ** -0.5, 0.25, ((0, 128),)),
        "low_v": centred(seeds[3], (LOW_MODES, NY), (LOW_MODES // 4) ** -0.5, 0.25, ((0, 128),)),
        "low_kx": draw_low_kx(jax.random.fold_in(seeds[7], 71), 0),
        "low_kz": draw_low_kz(jax.random.fold_in(seeds[7], 71), 0),
        "tau_inverse": centred(seeds[6], (LOW_MODES, NY, NY), NY ** -0.5, 0.25, ((0, 128),)),
    }


CONTRACT_FIRST = (((0,), (0,)), ((), ()))

def axis_table(index, positions, length):
    wavenum = jnp.where(index <= KL, index, index - KL)
    phases = wavenum[:, None] * positions[None, :] % length
    angles = phases.astype(jnp.float32) * (2.0 * math.pi / length)
    return jnp.where((index <= KL)[:, None], jnp.cos(angles), jnp.sin(angles))

def mode_weight(index_x, index_z):
    return jnp.where(index_x > 0, 2.0, 1.0).astype(jnp.float32) * jnp.where(index_z > 0, 2.0, 1.0).astype(jnp.float32)

def rounded(values):
    return lax.optimization_barrier(values.astype(jnp.bfloat16)).astype(jnp.float32)

def reference(high_u, high_v, low_u, low_v, low_kx, low_kz, tau_inverse):
    unitary = 1.0 / math.sqrt(NX * NZ)
    table_z = axis_table(low_kz, jnp.arange(NZ, dtype=jnp.int32), NZ)
    stacked = jnp.concatenate([low_u, low_v], axis=1).astype(jnp.float32)
    starts = jnp.arange(NX // CX, dtype=jnp.int32) * CX

    def patterns(offset):
        table_x = axis_table(low_kx, offset + jnp.arange(CX, dtype=jnp.int32), NX)
        return rounded((table_x[:, :, None] * table_z[:, None, :]).reshape(LOW_MODES, CX * NZ))

    def first_pass(offset):
        modes_table = patterns(offset)
        coarse = lax.dot_general(modes_table, stacked, CONTRACT_FIRST, preferred_element_type=jnp.float32)
        fine_u = lax.dynamic_slice_in_dim(high_u, offset, CX, 0).reshape(CX * NZ, NY).astype(jnp.float32)
        fine_v = lax.dynamic_slice_in_dim(high_v, offset, CX, 0).reshape(CX * NZ, NY).astype(jnp.float32)
        coarse_u = coarse[:, :NY]
        coarse_v = coarse[:, NY:]
        self_term = rounded(coarse_u * coarse_v + fine_u * fine_v)
        cross_term = coarse_u * fine_v + fine_u * coarse_v
        products = jnp.concatenate([self_term, rounded(cross_term)], axis=1)
        return (jnp.dot(modes_table, products, preferred_element_type=jnp.float32), cross_term)
    partials, cross_terms = lax.map(first_pass, starts)
    projected = lax.optimization_barrier(jnp.sum(partials, axis=0)) * unitary
    forcing = projected[:, :NY].astype(jnp.bfloat16)
    cross_low = (mode_weight(low_kx, low_kz)[:, None] * projected[:, NY:]).astype(jnp.bfloat16)

    def solve(operands):
        inverse_block, forcing_block = operands
        return jnp.einsum('mij,mj->mi', inverse_block.astype(jnp.float32), forcing_block.astype(jnp.float32))
    low_response = lax.map(solve, (tau_inverse.reshape(-1, LOW_DEV, NY, NY), forcing.reshape(-1, LOW_DEV, NY)))
    low_response = low_response.reshape(LOW_MODES, NY)
    cross_wide = cross_low.astype(jnp.float32)

    def second_pass(operands):
        offset, cross_term = operands
        restored = lax.dot_general(patterns(offset), cross_wide, CONTRACT_FIRST, preferred_element_type=jnp.float32)
        return (cross_term - unitary * restored).astype(jnp.bfloat16)
    high_term = lax.map(second_pass, (starts, cross_terms)).reshape(NX, NZ, NY)
    return (high_term, low_response)
```

```python
import math

import jax
import jax.numpy as jnp
from jax import lax
from jax.sharding import PartitionSpec as P

KL = 32
SIDE = 2 * KL + 1
LANES = 128
AXES = ("gx", "gz")
HIGH = lax.Precision.HIGH


def axis_table(index, positions, length):
    wavenum = jnp.where(index <= KL, index, index - KL)
    phases = wavenum[:, None] * positions[None, :] % length
    angles = phases.astype(jnp.float32) * (2.0 * math.pi / length)
    return jnp.where((index <= KL)[:, None], jnp.cos(angles), jnp.sin(angles))


def on_device(high_u, high_v, low_u, low_v, low_kx, low_kz, tau_inverse):
    cells_x, cells_z, levels = high_u.shape
    owned = low_u.shape[0]
    groups_x = lax.axis_size("gx")
    groups_z = lax.axis_size("gz")
    devices = groups_x * groups_z
    length_x = groups_x * cells_x
    length_z = groups_z * cells_z
    rows = levels // devices
    group = LANES // cells_z
    groups = cells_x // group
    unitary = 1.0 / math.sqrt(length_x * length_z)
    bf16 = jnp.bfloat16
    f32 = jnp.float32

    def to_rows(h):
        return h.reshape(groups, LANES, levels).transpose(2, 0, 1).reshape(
            devices, rows, groups, LANES
        )

    def low_rows(low):
        return low.reshape(owned, devices, rows).transpose(1, 2, 0)

    def everywhere(index):
        return jnp.broadcast_to(
            index.astype(bf16)[None, None, :], (devices, 2 * rows, owned)
        )

    values = jnp.concatenate([low_rows(low_u), low_rows(low_v)], axis=1)
    tile = jnp.concatenate([values, everywhere(low_kx), everywhere(low_kz)], axis=2)
    tile = jnp.pad(tile, ((0, 0), (0, 0), (0, LANES - 3 * owned)))
    sent = jnp.concatenate([to_rows(high_u), to_rows(high_v), tile[:, None]], axis=1)
    got = lax.all_to_all(sent, AXES, 0, 0, tiled=True)

    tile = got[:, 2 * rows]
    val = tile[:, :, :owned].transpose(0, 2, 1).reshape(-1, 2 * rows)
    kx = tile[:, 0, owned : 2 * owned].reshape(-1).astype(jnp.int32)
    kz = tile[:, 0, 2 * owned : 3 * owned].reshape(-1).astype(jnp.int32)
    indices = jnp.arange(SIDE, dtype=jnp.int32)
    pick_x = (kx[:, None] == indices[None, :]).astype(bf16)
    pick_z = (kz[:, None] == indices[None, :]).astype(bf16)
    spread = val[:, :, None] * pick_z[:, None, :]
    spectrum = jnp.einsum("ma,mcb->cab", pick_x, spread, preferred_element_type=f32)
    mask = jnp.einsum("ma,mb->ab", pick_x, pick_z, preferred_element_type=f32)
    table_x = axis_table(indices, jnp.arange(length_x, dtype=jnp.int32), length_x)
    table_z = axis_table(indices, jnp.arange(length_z, dtype=jnp.int32), length_z)

    def to_grid(coefficients):
        half = jnp.einsum("cab,ax->cxb", coefficients, table_x, precision=HIGH)
        return jnp.einsum("cxb,bz->cxz", half, table_z, precision=HIGH)

    fine = got[:, : 2 * rows].reshape(
        groups_x, groups_z, 2 * rows, groups, group, cells_z
    )
    fine = fine.transpose(2, 0, 3, 4, 1, 5).reshape(2 * rows, length_x, length_z)
    fine = fine.astype(f32)
    coarse = to_grid(spectrum)
    coarse_u, coarse_v = coarse[:rows], coarse[rows:]
    fine_u, fine_v = fine[:rows], fine[rows:]
    self_term = (coarse_u * coarse_v + fine_u * fine_v).astype(bf16)
    cross_term = coarse_u * fine_v + fine_u * coarse_v
    products = jnp.concatenate([self_term, cross_term.astype(bf16)], axis=0).astype(f32)
    half = jnp.einsum("cxz,bz->cxb", products, table_z, precision=HIGH)
    projected = jnp.einsum("cxb,ax->cab", half, table_x, precision=HIGH) * unitary
    twice = jnp.where(indices > 0, 2.0, 1.0).astype(f32)
    weight = twice[:, None] * twice[None, :]
    cross_low = (weight * projected[rows:]).astype(bf16).astype(f32) * mask
    high_term = (cross_term - unitary * to_grid(cross_low)).astype(bf16)
    high_term = high_term.reshape(rows, groups_x, groups, group, groups_z, cells_z)
    high_term = high_term.transpose(1, 4, 0, 2, 3, 5).reshape(
        devices, rows, groups, LANES
    )
    forcing = projected[:rows].astype(bf16)
    picked = jnp.einsum("ma,cab->mcb", pick_x, forcing, preferred_element_type=f32)
    picked = jnp.sum(picked * pick_z[:, None, :].astype(f32), axis=2).astype(bf16)
    picked = picked.reshape(devices, owned, rows).transpose(0, 2, 1)
    picked = jnp.pad(picked, ((0, 0), (0, groups - rows), (0, LANES - owned)))
    sent = jnp.concatenate([high_term, picked[:, None]], axis=1)
    got = lax.all_to_all(sent, AXES, 0, 0, tiled=True)

    high_term = got[:, :rows].reshape(levels, groups, LANES).transpose(1, 2, 0)
    high_term = high_term.reshape(cells_x, cells_z, levels)
    forcing = got[:, rows, :rows, :owned].reshape(levels, owned).T
    low_response = jnp.einsum(
        "mij,mj->mi", tau_inverse, forcing, preferred_element_type=f32
    )
    return (high_term, low_response)


def solution(mesh):
    placed = (
        P("gx", "gz", None),
        P("gx", "gz", None),
        P(AXES, None),
        P(AXES, None),
        P(AXES),
        P(AXES),
        P(AXES, None, None),
    )
    return jax.shard_map(
        on_device,
        mesh=mesh,
        in_specs=placed,
        out_specs=(P("gx", "gz", None), P(AXES, None)),
        check_vma=False,
    )
```

```python
import functools
import math

import jax
import jax.numpy as jnp
from jax import lax
from jax.experimental import pallas as pl
from jax.experimental.pallas import tpu as pltpu
from jax.sharding import PartitionSpec as P

KL = 32
SIDE = 2 * KL + 1
PADDED = 80
LANES = 128
HALF = LANES // 2
AXES = ("gx", "gz")
INTERPRET = False
VMEM_LIMIT = 48 * 1024 * 1024
bf16 = jnp.bfloat16
f32 = jnp.float32


def axis_table(index, positions, length):
    wavenum = jnp.where(index <= KL, index, index - KL)
    phases = wavenum[:, None] * positions[None, :] % length
    angles = phases.astype(f32) * (2.0 * math.pi / length)
    return jnp.where((index <= KL)[:, None], jnp.cos(angles), jnp.sin(angles))


def split(values):
    top = lax.reduce_precision(values, 8, 7)
    return top.astype(bf16), (values - top).astype(bf16)


def halves(values):
    top = values.astype(bf16)
    return top, (values - top.astype(f32)).astype(bf16)


def dot(a, b):
    return jnp.dot(a, b, preferred_element_type=f32)


def x_tables(groups_x, groups, group, length_x):
    part = jnp.arange(group, dtype=jnp.int32)[:, None, None]
    device = jnp.arange(groups_x, dtype=jnp.int32)[None, :, None]
    block = jnp.arange(groups, dtype=jnp.int32)[None, None, :]
    where_x = (device * (group * groups) + block * group + part).reshape(-1)
    index = jnp.arange(PADDED, dtype=jnp.int32)
    table = axis_table(index, where_x, length_x)
    table = jnp.where((index < SIDE)[:, None], table, 0.0)
    top, rest = split(table)
    forward = jnp.concatenate([top, rest], axis=0)
    top, rest = split(table.T)
    return forward, jnp.concatenate([top, rest], axis=1)


def z_tables(group, cells_z, length_z):
    column = jnp.arange(length_z * group, dtype=jnp.int32)
    where_z = column // (group * cells_z) * cells_z + column % cells_z
    owner = column // cells_z % group
    index = jnp.arange(1, SIDE, dtype=jnp.int32)
    table = axis_table(index, where_z, length_z)
    part = jnp.arange(group, dtype=jnp.int32)
    inverse = jnp.where(part[:, None, None] == owner[None, None, :], table[None], 0.0)
    inverse = inverse.reshape(group * HALF, -1)
    forward = jnp.where(
        part[None, :, None] == owner[:, None, None], table.T[:, None, :], 0.0
    )
    forward = forward.reshape(-1, group * HALF)
    return split(inverse), jnp.concatenate(split(forward), axis=1)


def prepare_kernel(u_ref, v_ref, low_u_ref, low_v_ref, index_ref, out_ref, tall, low, tile):
    groups = u_ref.shape[0]
    levels = u_ref.shape[2]
    devices = out_ref.shape[0]
    rows = levels // devices
    step = rows * groups
    side = 2 * LANES
    eye = (
        lax.broadcasted_iota(jnp.int32, (side, side), 0)
        == lax.broadcasted_iota(jnp.int32, (side, side), 1)
    ).astype(bf16)
    for k, ref in enumerate((u_ref, v_ref)):
        for g in range(0, groups, 2):
            block = ref[g : g + 2].reshape(side, levels)
            for y in range(0, levels, side):
                turned = lax.dot_general(
                    eye,
                    block[:, y : y + side],
                    (((1,), (1,)), ((), ())),
                    preferred_element_type=f32,
                )
                tall[pl.ds(y * groups + g, side, stride=groups), :] = turned[:, :LANES]
                tall[pl.ds(y * groups + g + 1, side, stride=groups), :] = turned[:, LANES:]
        out_ref[:, k * step : (k + 1) * step, :] = (
            tall[...].astype(bf16).reshape(devices, step, LANES)
        )
    eye = eye[:LANES, :LANES]
    owned = low_u_ref.shape[0]
    for k, ref in enumerate((low_u_ref, low_v_ref)):
        padded = jnp.concatenate(
            [ref[...].astype(f32), jnp.zeros((LANES - owned, levels), f32)], axis=0
        ).astype(bf16)
        for y in range(0, levels, LANES):
            low[pl.ds(y, LANES), :] = lax.dot_general(
                eye,
                padded[:, y : y + LANES],
                (((1,), (1,)), ((), ())),
                preferred_element_type=f32,
            )
        for y in range(rows):
            tile[pl.ds(k * rows + y, devices, stride=groups), :] = (
                low[pl.ds(y, devices, stride=rows), :] + index_ref[...]
            )
    out_ref[:, 2 * step :, :] = tile[...].astype(bf16).reshape(devices, groups, LANES)


def middle_kernel(
    unitary,
    got_ref,
    back_x_ref,
    x_ref,
    top_ref,
    rest_ref,
    z_ref,
    out_ref,
    modes,
    left,
    right,
    spectrum,
    wave,
    mean,
    wave_top,
    wave_rest,
    products,
    sums,
    cross,
    coefficients,
    picked,
):
    groups_x, groups_z, _, _ = got_ref.shape
    groups = 8
    rows = 4
    owned = 16
    devices = groups_x * groups_z
    step = rows * groups
    points = groups_x * groups
    side = 2 * LANES
    lane = lax.broadcasted_iota(jnp.int32, (1, LANES), 1)
    low_half = lane < HALF

    modes[...] = got_ref[:, :, 2 * step :, :].astype(f32).reshape(devices * groups, LANES)
    first = modes[pl.ds(0, devices, stride=groups), :]
    turned = [first.T]
    for c in range(1, 2 * rows):
        turned.append(modes[pl.ds(c, devices, stride=groups), :].T)
    row = lax.broadcasted_iota(jnp.int32, (PADDED, devices), 0).astype(f32)
    column = lax.broadcasted_iota(jnp.int32, (devices, LANES), 1)
    wanted = (1 + column % HALF).astype(f32)
    for m in range(owned):
        at = slice(m * devices, (m + 1) * devices)
        hit = row == turned[0][owned + m : owned + m + 1, :]
        for c in range(2 * rows):
            left[c * PADDED : (c + 1) * PADDED, at] = jnp.where(
                hit, turned[c][m : m + 1, :], 0.0
            ).astype(bf16)
        left[2 * rows * PADDED :, at] = jnp.where(hit, 1.0, 0.0).astype(bf16)
        index_z = first[:, 2 * owned + m : 2 * owned + m + 1]
        right[at, :LANES] = jnp.where(wanted == index_z, 1.0, 0.0).astype(bf16)
        right[at, LANES:] = jnp.where(
            jnp.zeros((devices, LANES), f32) == index_z, 1.0, 0.0
        ).astype(bf16)
    spectrum[...] = dot(left[...], right[...]).astype(bf16)

    def spread(coefficient):
        full = dot(back_x_ref[...], jnp.concatenate([coefficient] * 2, axis=0))
        parts = [full[k * points : (k + 1) * points] for k in range(4)]
        waves = jnp.concatenate(
            [
                jnp.where(low_half, parts[0][:, :LANES], parts[1][:, :LANES]),
                jnp.where(low_half, parts[2][:, :LANES], parts[3][:, :LANES]),
            ],
            axis=1,
        )
        which = lane // (LANES // 4)
        constant = parts[3][:, LANES:]
        for k in range(3):
            constant = jnp.where(which == k, parts[k][:, LANES:], constant)
        return (
            waves.reshape(groups_x, groups, side),
            constant.reshape(groups_x, groups, LANES),
        )

    for c in range(2 * rows):
        waves, constant = spread(spectrum[c * PADDED : (c + 1) * PADDED, :])
        wave[c // rows, :, c % rows] = waves
        mean[c // rows, :, c % rows] = constant
    top, rest = halves(wave[...].reshape(2 * groups_x * step, side))
    wave_top[...] = top
    wave_rest[...] = rest
    sums[...] = jnp.zeros_like(sums)
    half_rows = groups_x * step

    def fine(j, k):
        parts = [
            got_ref[:, 2 * j + e, k * step : (k + 1) * step, :].reshape(half_rows, LANES)
            for e in range(2)
        ]
        return jnp.concatenate(parts, axis=1).astype(f32)

    def multiply(j, _):
        at = pl.ds(pl.multiple_of(j * side, side), side)
        coarse = (
            dot(wave_top[...], top_ref[:, at])
            + dot(wave_rest[...], top_ref[:, at])
            + dot(wave_top[...], rest_ref[:, at])
        )
        flat = mean[...].reshape(2 * half_rows, LANES)
        coarse = coarse + jnp.concatenate([flat, flat], axis=1)
        coarse_u, coarse_v = coarse[:half_rows], coarse[half_rows:]
        fine_u, fine_v = fine(j, 0), fine(j, 1)
        self_term = (coarse_u * coarse_v + fine_u * fine_v).astype(bf16)
        cross_term = coarse_u * fine_v + fine_u * coarse_v
        cross[:, at] = cross_term
        cross_round = cross_term.astype(bf16)
        products[:half_rows, at] = self_term
        products[half_rows:, at] = cross_round
        for k, term in enumerate((self_term, cross_round)):
            wide = term.astype(f32)
            sums[k] += (wide[:, :LANES] + wide[:, LANES:]).reshape(
                groups_x, rows, groups, LANES
            )
        return 0

    lax.fori_loop(0, groups_z // 2, multiply, 0)
    both = dot(products[...], z_ref[...])
    coefficients[...] = (both[:, :side] + both[:, side:]).reshape(
        2, groups_x, rows, groups, side
    )

    def project(k, y):
        waves = coefficients[k, :, y].reshape(points, side)
        total = sums[k, :, y].reshape(points, LANES)
        stack = []
        for part in range(4):
            half = waves[:, :LANES] if part < 2 else waves[:, LANES:]
            keep = low_half if part % 2 == 0 else jnp.logical_not(low_half)
            stack.append(
                jnp.concatenate(
                    [
                        jnp.where(keep, half, 0.0),
                        jnp.where(lane // (LANES // 4) == part, total, 0.0),
                    ],
                    axis=1,
                )
            )
        top, rest = halves(jnp.concatenate(stack, axis=0))
        outer = dot(x_ref[...], top)
        outer = outer[:PADDED] + outer[PADDED:] + dot(x_ref[:PADDED], rest)
        waves = outer[:, :LANES] * unitary
        waves = waves + pltpu.roll(waves, HALF, 1)
        constant = jnp.sum(outer[:, LANES:], axis=1, keepdims=True) * unitary
        return waves, jnp.broadcast_to(constant, (PADDED, LANES))

    row_index = lax.broadcasted_iota(jnp.int32, (PADDED, 1), 0)
    weight_x = jnp.where(row_index > 0, 2.0, 1.0).astype(f32)
    mask = spectrum[2 * rows * PADDED :, :]
    for y in range(rows):
        waves, constant = project(1, y)
        low = jnp.concatenate([waves * (2.0 * weight_x), constant * weight_x], axis=1)
        waves, constant = spread(low.astype(bf16) * mask)
        wave[0, :, y] = waves
        mean[0, :, y] = constant
    top, rest = halves(wave[0].reshape(half_rows, side))
    wave_top[:half_rows] = top
    wave_rest[:half_rows] = rest

    def subtract(j, _):
        at = pl.ds(pl.multiple_of(j * side, side), side)
        restored = dot(wave_top[:half_rows], top_ref[:, at]) + dot(
            wave_rest[:half_rows], top_ref[:, at]
        )
        flat = mean[0].reshape(half_rows, LANES)
        restored = restored + jnp.concatenate([flat, flat], axis=1)
        high = (cross[:, at] - unitary * restored).astype(bf16)
        for e in range(2):
            out_ref[:, 2 * j + e, :step, :] = high[:, e * LANES : (e + 1) * LANES].reshape(
                groups_x, step, LANES
            )
        return 0

    lax.fori_loop(0, groups_z // 2, subtract, 0)

    lines = 72
    parts = []
    for y in range(rows):
        waves, constant = project(0, y)
        force = jnp.where(low_half, waves, jnp.where(lane == HALF, constant, 0.0))
        force = jnp.concatenate([force, jnp.zeros((LANES - PADDED, LANES), f32)], axis=0)
        parts.append(force.T[:lines])
    force = jnp.concatenate(parts, axis=0).astype(bf16)[:, :PADDED]
    line = lax.broadcasted_iota(jnp.int32, (lines, devices), 0)
    line = jnp.where(line < HALF, line + 1, jnp.where(line == HALF, 0, -1)).astype(f32)
    picked[...] = jnp.zeros_like(picked)
    for m in range(0, owned, 2):
        chosen = dot(force, left[2 * rows * PADDED :, m * devices : (m + 2) * devices])
        for e in range(2):
            hit = line == turned[0][2 * owned + m + e : 2 * owned + m + e + 1, :]
            for y in range(rows):
                value = chosen[y * lines : (y + 1) * lines, e * devices : (e + 1) * devices]
                picked[y, m + e : m + e + 1, :] = jnp.sum(
                    jnp.where(hit, value, 0.0), axis=0, keepdims=True
                )
    modes[...] = jnp.zeros_like(modes)
    for y in range(rows):
        modes[pl.ds(y, devices, stride=groups), :] = picked[y].T
    out_ref[:, :, step:, :] = (
        modes[...].astype(bf16).reshape(groups_x, groups_z, groups, LANES)
    )


def on_device(high_u, high_v, low_u, low_v, low_kx, low_kz, tau_inverse):
    cells_x, cells_z, levels = high_u.shape
    owned = low_u.shape[0]
    groups_x = lax.axis_size("gx")
    groups_z = lax.axis_size("gz")
    devices = groups_x * groups_z
    length_x = groups_x * cells_x
    length_z = groups_z * cells_z
    rows = levels // devices
    group = LANES // cells_z
    groups = cells_x // group
    step = rows * groups
    points = groups_x * groups
    half_rows = groups_x * step
    width = groups_z * LANES
    side = 2 * LANES
    unitary = 1.0 / math.sqrt(length_x * length_z)

    index = jnp.concatenate(
        [jnp.zeros((owned,), f32), low_kx.astype(f32), low_kz.astype(f32)]
    )
    index = jnp.pad(index, (0, LANES - 3 * owned))[None, :]
    sent = pl.pallas_call(
        prepare_kernel,
        out_shape=jax.ShapeDtypeStruct((devices, 2 * step + groups, LANES), bf16),
        scratch_shapes=[
            pltpu.VMEM((levels * groups, LANES), f32),
            pltpu.VMEM((levels, LANES), f32),
            pltpu.VMEM((devices * groups, LANES), f32),
        ],
        compiler_params=pltpu.CompilerParams(vmem_limit_bytes=VMEM_LIMIT),
        interpret=INTERPRET,
        name="prepare",
    )(
        high_u.reshape(groups, LANES, levels),
        high_v.reshape(groups, LANES, levels),
        low_u,
        low_v,
        index,
    )
    got = lax.all_to_all(sent, AXES, 0, 0, tiled=True)

    forward_x, back_x = x_tables(groups_x, groups, group, length_x)
    (top, rest), forward_z = z_tables(group, cells_z, length_z)
    sent = pl.pallas_call(
        functools.partial(middle_kernel, unitary),
        out_shape=jax.ShapeDtypeStruct((groups_x, groups_z, step + groups, LANES), bf16),
        scratch_shapes=[
            pltpu.VMEM((devices * groups, LANES), f32),
            pltpu.VMEM(((2 * rows + 1) * PADDED, owned * devices), bf16),
            pltpu.VMEM((owned * devices, side), bf16),
            pltpu.VMEM(((2 * rows + 1) * PADDED, side), bf16),
            pltpu.VMEM((2, groups_x, rows, groups, side), f32),
            pltpu.VMEM((2, groups_x, rows, groups, LANES), f32),
            pltpu.VMEM((2 * half_rows, side), bf16),
            pltpu.VMEM((2 * half_rows, side), bf16),
            pltpu.VMEM((2 * half_rows, width), bf16),
            pltpu.VMEM((2, groups_x, rows, groups, LANES), f32),
            pltpu.VMEM((half_rows, width), f32),
            pltpu.VMEM((2, groups_x, rows, groups, side), f32),
            pltpu.VMEM((rows, LANES, devices), f32),
        ],
        compiler_params=pltpu.CompilerParams(vmem_limit_bytes=VMEM_LIMIT),
        interpret=INTERPRET,
        name="middle",
    )(
        got.reshape(groups_x, groups_z, 2 * step + groups, LANES),
        back_x,
        forward_x,
        top,
        rest,
        forward_z,
    )
    got = lax.all_to_all(
        sent.reshape(devices, step + groups, LANES), AXES, 0, 0, tiled=True
    )

    high_term = got[:, :step].reshape(levels, groups, LANES).transpose(1, 2, 0)
    high_term = high_term.reshape(cells_x, cells_z, levels)
    forcing = got[:, step : step + rows, :owned].reshape(levels, owned).T
    low_response = jnp.einsum(
        "mij,mj->mi", tau_inverse, forcing, preferred_element_type=f32
    )
    return (high_term, low_response)


def solution(mesh):
    placed = (
        P("gx", "gz", None),
        P("gx", "gz", None),
        P(AXES, None),
        P(AXES, None),
        P(AXES),
        P(AXES),
        P(AXES, None, None),
    )
    return jax.shard_map(
        on_device,
        mesh=mesh,
        in_specs=placed,
        out_specs=(P("gx", "gz", None), P(AXES, None)),
        check_vma=False,
    )
```

```python
import functools
import math

import jax
import jax.numpy as jnp
from jax import lax
from jax.experimental import pallas as pl
from jax.experimental.pallas import tpu as pltpu
from jax.sharding import PartitionSpec as P

KL = 32
SIDE = 2 * KL + 1
PADDED = 80
LANES = 128
HALF = LANES // 2
AXES = ("gx", "gz")
INTERPRET = False
WHOLE = 67043328
UNROLL = 1
bf16 = jnp.bfloat16
f32 = jnp.float32


def axis_table(index, positions, length):
    wavenum = jnp.where(index <= KL, index, index - KL)
    phases = wavenum[:, None] * positions[None, :] % length
    angles = phases.astype(f32) * (2.0 * math.pi / length)
    return jnp.where((index <= KL)[:, None], jnp.cos(angles), jnp.sin(angles))


def split(values):
    top = lax.reduce_precision(values, 8, 7)
    return top.astype(bf16), (values - top).astype(bf16)


def halves(values):
    top = values.astype(bf16)
    return top, (values - top.astype(f32)).astype(bf16)


def dot(a, b):
    return jnp.dot(a, b, preferred_element_type=f32)


def x_tables(groups_x, groups, group, length_x):
    part = jnp.arange(group, dtype=jnp.int32)[:, None, None]
    device = jnp.arange(groups_x, dtype=jnp.int32)[None, :, None]
    block = jnp.arange(groups, dtype=jnp.int32)[None, None, :]
    where_x = (device * (group * groups) + block * group + part).reshape(-1)
    index = jnp.arange(PADDED, dtype=jnp.int32)
    table = axis_table(index, where_x, length_x)
    table = jnp.where((index < SIDE)[:, None], table, 0.0)
    top, rest = split(table)
    forward = jnp.concatenate([top, rest], axis=0)
    top, rest = split(table.T)
    return forward, jnp.concatenate([top, rest], axis=1)


def z_tables(group, cells_z, length_z):
    column = jnp.arange(length_z * group, dtype=jnp.int32)
    where_z = column // (group * cells_z) * cells_z + column % cells_z
    owner = column // cells_z % group
    index = jnp.arange(1, SIDE, dtype=jnp.int32)
    table = axis_table(index, where_z, length_z)
    part = jnp.arange(group, dtype=jnp.int32)
    inverse = jnp.where(part[:, None, None] == owner[None, None, :], table[None], 0.0)
    inverse = inverse.reshape(group * HALF, -1)
    forward = jnp.where(
        part[None, :, None] == owner[:, None, None], table.T[:, None, :], 0.0
    )
    forward = forward.reshape(-1, group * HALF)
    return inverse.astype(bf16), split(forward)


def across(eye, block):
    return lax.dot_general(
        eye, block, (((1,), (1,)), ((), ())), preferred_element_type=f32
    )


def identity(size):
    return (
        lax.broadcasted_iota(jnp.int32, (size, size), 0)
        == lax.broadcasted_iota(jnp.int32, (size, size), 1)
    ).astype(bf16)


def prepare_kernel(
    u_ref,
    v_ref,
    low_u_ref,
    low_v_ref,
    kx_ref,
    kz_ref,
    out_ref,
    fine,
    lows,
    index,
    tall,
    low,
    tile,
    ready,
    fine_sem,
    low_sem,
    index_sem,
    out_sem,
):
    groups, _, levels = u_ref.shape
    owned = low_u_ref.shape[0]
    devices = out_ref.shape[0]
    rows = levels // devices
    step = rows * groups
    side = 2 * LANES
    pairs = groups // 2
    copies = []
    for k, ref in enumerate((kx_ref, kz_ref)):
        copies.append(pltpu.make_async_copy(ref, index.at[k], index_sem.at[k]))
    for k, ref in enumerate((low_u_ref, low_v_ref)):
        copies.append(pltpu.make_async_copy(ref, lows.at[k], low_sem.at[k]))
    for k, ref in enumerate((u_ref, v_ref)):
        for g in range(pairs):
            at = pl.ds(2 * g, 2)
            copies.append(
                pltpu.make_async_copy(ref.at[at], fine.at[k, at], fine_sem.at[k, g])
            )
    for copy in copies:
        copy.start()
    for copy in copies[:4]:
        copy.wait()

    def send(k, first, count):
        part = (slice(None), pl.ds(first, count))
        return pltpu.make_async_copy(ready.at[part], out_ref.at[part], out_sem.at[k])

    lane = lax.broadcasted_iota(jnp.int32, (1, LANES), 1)
    line = jnp.zeros((1, LANES), f32)
    for m in range(owned):
        line = jnp.where(lane == owned + m, index[0, m].astype(f32), line)
        line = jnp.where(lane == 2 * owned + m, index[1, m].astype(f32), line)
    eye = identity(LANES)
    for k in range(2):
        padded = jnp.concatenate(
            [lows[k].astype(f32), jnp.zeros((LANES - owned, levels), f32)], axis=0
        ).astype(bf16)
        for y in range(0, levels, LANES):
            low[pl.ds(y, LANES), :] = across(eye, padded[:, y : y + LANES])
        for y in range(rows):
            tile[pl.ds(k * rows + y, devices, stride=groups), :] = (
                low[pl.ds(y, devices, stride=rows), :] + line
            )
    ready[:, 2 * step :, :] = tile[...].astype(bf16).reshape(devices, groups, LANES)
    sends = [send(2, 2 * step, groups)]
    sends[0].start()
    eye = identity(side)
    for k in range(2):
        for g in range(pairs):
            copies[4 + k * pairs + g].wait()
            block = fine[k, 2 * g : 2 * g + 2].reshape(side, levels)
            for y in range(0, levels, side):
                turned = across(eye, block[:, y : y + side])
                at = y * groups + 2 * g
                tall[pl.ds(at, side, stride=groups), :] = turned[:, :LANES]
                tall[pl.ds(at + 1, side, stride=groups), :] = turned[:, LANES:]
        ready[:, k * step : (k + 1) * step, :] = (
            tall[...].astype(bf16).reshape(devices, step, LANES)
        )
        sends.append(send(k, k * step, step))
        sends[-1].start()
    for copy in sends:
        copy.wait()


def middle_kernel(
    unitary,
    got_hbm,
    back_x_hbm,
    x_hbm,
    top_hbm,
    z_top_hbm,
    z_rest_hbm,
    out_hbm,
    got_ref,
    back_x_ref,
    x_ref,
    top_ref,
    z_top_ref,
    z_rest_ref,
    out_ref,
    modes,
    left,
    right,
    spectrum,
    wave,
    mean,
    wave_top,
    products,
    sums,
    cross,
    coefficients,
    picked,
    in_sem,
    out_sem,
):
    groups_x, groups_z, _, _ = got_ref.shape
    groups = 8
    rows = 4
    owned = 16
    devices = groups_x * groups_z
    step = rows * groups
    points = groups_x * groups
    side = 2 * LANES
    half_rows = groups_x * step
    lane = lax.broadcasted_iota(jnp.int32, (1, LANES), 1)
    low_half = lane < HALF
    which = lane // (LANES // 4)

    everything = (slice(None), slice(None))
    tiles = everything + (pl.ds(2 * step, groups),)
    lines = everything + (pl.ds(0, 2 * step),)
    fetches = [
        pltpu.make_async_copy(source, target, in_sem.at[k])
        for k, (source, target) in enumerate(
            (
                (got_hbm.at[tiles], got_ref.at[tiles]),
                (back_x_hbm, back_x_ref),
                (top_hbm, top_ref),
                (got_hbm.at[lines], got_ref.at[lines]),
                (x_hbm, x_ref),
                (z_top_hbm, z_top_ref),
                (z_rest_hbm, z_rest_ref),
            )
        )
    ]
    for fetch in fetches:
        fetch.start()
    fetches[0].wait()
    modes[...] = got_ref[:, :, 2 * step :, :].astype(f32).reshape(devices * groups, LANES)
    first = modes[pl.ds(0, devices, stride=groups), :]
    turned = [first.T]
    for c in range(1, 2 * rows):
        turned.append(modes[pl.ds(c, devices, stride=groups), :].T)
    row = lax.broadcasted_iota(jnp.int32, (PADDED, devices), 0).astype(f32)
    column = lax.broadcasted_iota(jnp.int32, (devices, LANES), 1)
    wanted = (1 + column % HALF).astype(f32)
    for m in range(owned):
        at = slice(m * devices, (m + 1) * devices)
        hit = row == turned[0][owned + m : owned + m + 1, :]
        hit = jnp.where(hit, 1.0, 0.0).astype(bf16)
        for c in range(2 * rows):
            value = jnp.broadcast_to(turned[c][m : m + 1, :], (16, devices)).astype(bf16)
            value = jnp.concatenate([value] * (PADDED // 16), axis=0)
            left[c * PADDED : (c + 1) * PADDED, at] = hit * value
        left[2 * rows * PADDED :, at] = hit
        index_z = jnp.broadcast_to(
            first[:, 2 * owned + m : 2 * owned + m + 1], (devices, LANES)
        )
        right[at, :LANES] = jnp.where(wanted == index_z, 1.0, 0.0).astype(bf16)
        right[at, LANES:] = jnp.where(index_z == 0.0, 1.0, 0.0).astype(bf16)
    spectrum[...] = dot(left[...], right[...]).astype(bf16)
    fetches[1].wait()

    def spread(k, parts):
        both = jnp.concatenate(parts, axis=1)
        full = dot(back_x_ref[...], jnp.concatenate([both, both], axis=0))
        for y in range(len(parts)):
            part = [
                full[p * points : (p + 1) * points, y * side : (y + 1) * side]
                for p in range(4)
            ]
            waves = jnp.concatenate(
                [
                    jnp.where(low_half, part[0][:, :LANES], part[1][:, :LANES]),
                    jnp.where(low_half, part[2][:, :LANES], part[3][:, :LANES]),
                ],
                axis=1,
            )
            constant = part[3][:, LANES:]
            for p in range(3):
                constant = jnp.where(which == p, part[p][:, LANES:], constant)
            wave[k, :, y] = waves.reshape(groups_x, groups, side)
            mean[k, :, y] = constant.reshape(groups_x, groups, LANES)

    for k in range(2):
        spread(
            k,
            [
                spectrum[(k * rows + y) * PADDED : (k * rows + y + 1) * PADDED, :]
                for y in range(rows)
            ],
        )
    wave_top[...] = wave[...].reshape(2 * half_rows, side).astype(bf16)
    sums[...] = jnp.zeros_like(sums)
    fetches[2].wait()
    fetches[3].wait()

    def fine(j, k):
        parts = [
            got_ref[:, 2 * j + e, k * step : (k + 1) * step, :].reshape(half_rows, LANES)
            for e in range(2)
        ]
        return jnp.concatenate(parts, axis=1).astype(f32)

    def multiply(j, _):
        at = pl.ds(pl.multiple_of(j * side, side), side)
        coarse = dot(wave_top[...], top_ref[:, at])
        flat = mean[...].reshape(2 * half_rows, LANES)
        coarse = coarse + jnp.concatenate([flat, flat], axis=1)
        coarse_u, coarse_v = coarse[:half_rows], coarse[half_rows:]
        fine_u, fine_v = fine(j, 0), fine(j, 1)
        self_term = (coarse_u * coarse_v + fine_u * fine_v).astype(bf16)
        cross_term = coarse_u * fine_v + fine_u * coarse_v
        cross[:, at] = cross_term
        cross_round = cross_term.astype(bf16)
        products[:half_rows, at] = self_term
        products[half_rows:, at] = cross_round
        for k, term in enumerate((self_term, cross_round)):
            wide = term.astype(f32)
            sums[k] += (wide[:, :LANES] + wide[:, LANES:]).reshape(
                groups_x, rows, groups, LANES
            )
        return 0

    lax.fori_loop(0, groups_z // 2, multiply, 0, unroll=UNROLL)
    for fetch in fetches[4:]:
        fetch.wait()
    both = dot(products[...], z_top_ref[...]) + dot(products[...], z_rest_ref[...])
    coefficients[...] = both.reshape(2, groups_x, rows, groups, side)

    def project(k):
        stacks = []
        for y in range(rows):
            waves = coefficients[k, :, y].reshape(points, side)
            total = sums[k, :, y].reshape(points, LANES)
            stack = []
            for part in range(4):
                half = waves[:, :LANES] if part < 2 else waves[:, LANES:]
                keep = low_half if part % 2 == 0 else jnp.logical_not(low_half)
                stack.append(
                    jnp.concatenate(
                        [
                            jnp.where(keep, half, 0.0),
                            jnp.where(which == part, total, 0.0),
                        ],
                        axis=1,
                    )
                )
            stacks.append(jnp.concatenate(stack, axis=0))
        top, rest = halves(jnp.concatenate(stacks, axis=1))
        outer = dot(x_ref[...], top)
        outer = outer[:PADDED] + outer[PADDED:] + dot(x_ref[:PADDED], rest)
        done = []
        for y in range(rows):
            waves = outer[:, y * side : y * side + LANES] * unitary
            waves = waves + pltpu.roll(waves, HALF, 1)
            constant = outer[:, y * side + LANES : (y + 1) * side]
            constant = jnp.sum(constant, axis=1, keepdims=True) * unitary
            done.append((waves, jnp.broadcast_to(constant, (PADDED, LANES))))
        return done

    row_index = lax.broadcasted_iota(jnp.int32, (PADDED, 1), 0)
    weight_x = jnp.where(row_index > 0, 2.0, 1.0).astype(f32)
    mask = spectrum[2 * rows * PADDED :, :]
    parts = []
    for waves, constant in project(1):
        low = jnp.concatenate([waves * (2.0 * weight_x), constant * weight_x], axis=1)
        parts.append(low.astype(bf16) * mask)
    spread(0, parts)
    wave_top[:half_rows] = wave[0].reshape(half_rows, side).astype(bf16)

    kept = 72
    parts = []
    for waves, constant in project(0):
        force = jnp.where(low_half, waves, jnp.where(lane == HALF, constant, 0.0))
        force = jnp.concatenate([force, jnp.zeros((LANES - PADDED, LANES), f32)], axis=0)
        parts.append(force.T[:kept])
    force = jnp.concatenate(parts, axis=0).astype(bf16)[:, :PADDED]
    line = lax.broadcasted_iota(jnp.int32, (kept, devices), 0)
    line = jnp.where(line < HALF, line + 1, jnp.where(line == HALF, 0, -1)).astype(f32)
    picked[...] = jnp.zeros_like(picked)
    for m in range(0, owned, 2):
        chosen = dot(force, left[2 * rows * PADDED :, m * devices : (m + 2) * devices])
        for e in range(2):
            hit = line == turned[0][2 * owned + m + e : 2 * owned + m + e + 1, :]
            for y in range(rows):
                value = chosen[y * kept : (y + 1) * kept, e * devices : (e + 1) * devices]
                picked[y, m + e : m + e + 1, :] = jnp.sum(
                    jnp.where(hit, value, 0.0), axis=0, keepdims=True
                )
    modes[...] = jnp.zeros_like(modes)
    for y in range(rows):
        modes[pl.ds(y, devices, stride=groups), :] = picked[y].T
    out_ref[:, :, step:, :] = (
        modes[...].astype(bf16).reshape(groups_x, groups_z, groups, LANES)
    )
    part = everything + (pl.ds(step, groups),)
    send_tiles = pltpu.make_async_copy(
        out_ref.at[part], out_hbm.at[part], out_sem.at[groups_z // 2]
    )
    send_tiles.start()

    def send(j):
        part = (slice(None), pl.ds(2 * j, 2), pl.ds(0, step))
        return pltpu.make_async_copy(out_ref.at[part], out_hbm.at[part], out_sem.at[j])

    def subtract(j, _):
        at = pl.ds(pl.multiple_of(j * side, side), side)
        restored = dot(wave_top[:half_rows], top_ref[:, at])
        flat = mean[0].reshape(half_rows, LANES)
        restored = restored + jnp.concatenate([flat, flat], axis=1)
        high = (cross[:, at] - unitary * restored).astype(bf16)
        for e in range(2):
            out_ref[:, 2 * j + e, :step, :] = high[:, e * LANES : (e + 1) * LANES].reshape(
                groups_x, step, LANES
            )
        send(j).start()
        return 0

    lax.fori_loop(0, groups_z // 2, subtract, 0, unroll=UNROLL)
    send_tiles.wait()

    def drain(j, _):
        send(j).wait()
        return 0

    lax.fori_loop(0, groups_z // 2, drain, 0)


def finish_kernel(
    got_hbm,
    tau_hbm,
    high_hbm,
    low_ref,
    got_ref,
    tau_ref,
    tall,
    tile,
    force,
    ready,
    got_sem,
    tau_sem,
    out_sem,
):
    devices = got_hbm.shape[0]
    owned, levels, _ = tau_hbm.shape
    rows = levels // devices
    groups = high_hbm.shape[0]
    step = rows * groups
    chunk = LANES // rows
    count = devices // chunk
    fetches = []
    for q in range(count):
        at = pl.ds(q * chunk, chunk)
        fetches.append(
            pltpu.make_async_copy(got_hbm.at[at], got_ref.at[at], got_sem.at[q])
        )
    for m in range(owned):
        fetches.append(
            pltpu.make_async_copy(tau_hbm.at[m], tau_ref.at[m], tau_sem.at[m])
        )
    for fetch in fetches:
        fetch.start()
    eye = identity(LANES)
    sends = []
    for q in range(count):
        fetches[q].wait()
        at = slice(q * chunk, (q + 1) * chunk)
        tall[...] = got_ref[at, :step, :].astype(f32).reshape(chunk * step, LANES)
        where = pl.ds(q * LANES, LANES)
        for g in range(groups):
            column = tall[pl.ds(g, LANES, stride=groups), :].astype(bf16)
            ready[g, :, q * LANES : (q + 1) * LANES] = across(eye, column).astype(bf16)
        part = (slice(None), slice(None), where)
        sends.append(
            pltpu.make_async_copy(ready.at[part], high_hbm.at[part], out_sem.at[q])
        )
        sends[-1].start()
    tile[...] = got_ref[:, step:, :].astype(f32).reshape(devices * groups, LANES)
    for y in range(rows):
        force[pl.ds(y, devices, stride=rows), :] = tile[
            pl.ds(y, devices, stride=groups), :
        ]
    vector = force[...].astype(bf16)
    lane = lax.broadcasted_iota(jnp.int32, (levels, LANES), 1)
    answer = jnp.zeros((levels, LANES), f32)
    for m in range(owned):
        fetches[count + m].wait()
        answer = jnp.where(lane == m, dot(tau_ref[m], vector), answer)
    low_ref[...] = answer.T[:owned]
    for copy in sends:
        copy.wait()


def on_device(high_u, high_v, low_u, low_v, low_kx, low_kz, tau_inverse):
    cells_x, cells_z, levels = high_u.shape
    owned = low_u.shape[0]
    groups_x = lax.axis_size("gx")
    groups_z = lax.axis_size("gz")
    devices = groups_x * groups_z
    length_x = groups_x * cells_x
    length_z = groups_z * cells_z
    rows = levels // devices
    group = LANES // cells_z
    groups = cells_x // group
    step = rows * groups
    points = groups_x * groups
    half_rows = groups_x * step
    width = groups_z * LANES
    side = 2 * LANES
    unitary = 1.0 / math.sqrt(length_x * length_z)

    anywhere = pl.BlockSpec(memory_space=pltpu.HBM)
    sent = pl.pallas_call(
        prepare_kernel,
        out_shape=jax.ShapeDtypeStruct((devices, 2 * step + groups, LANES), bf16),
        in_specs=[anywhere] * 6,
        out_specs=anywhere,
        scratch_shapes=[
            pltpu.VMEM((2, groups, LANES, levels), bf16),
            pltpu.VMEM((2, owned, levels), bf16),
            pltpu.SMEM((2, owned), jnp.int32),
            pltpu.VMEM((levels * groups, LANES), f32),
            pltpu.VMEM((levels, LANES), f32),
            pltpu.VMEM((devices * groups, LANES), f32),
            pltpu.VMEM((devices, 2 * step + groups, LANES), bf16),
            pltpu.SemaphoreType.DMA((2, groups // 2)),
            pltpu.SemaphoreType.DMA((2,)),
            pltpu.SemaphoreType.DMA((2,)),
            pltpu.SemaphoreType.DMA((3,)),
        ],
        compiler_params=pltpu.CompilerParams(vmem_limit_bytes=WHOLE),
        interpret=INTERPRET,
        name="prepare",
    )(
        high_u.reshape(groups, LANES, levels),
        high_v.reshape(groups, LANES, levels),
        low_u,
        low_v,
        low_kx,
        low_kz,
    )
    got = lax.all_to_all(sent, AXES, 0, 0, tiled=True)

    forward_x, back_x = x_tables(groups_x, groups, group, length_x)
    top, forward_z = z_tables(group, cells_z, length_z)
    sent = pl.pallas_call(
        functools.partial(middle_kernel, unitary),
        out_shape=jax.ShapeDtypeStruct((groups_x, groups_z, step + groups, LANES), bf16),
        in_specs=[anywhere] * 6,
        out_specs=anywhere,
        scratch_shapes=[
            pltpu.VMEM((groups_x, groups_z, 2 * step + groups, LANES), bf16),
            pltpu.VMEM(back_x.shape, bf16),
            pltpu.VMEM(forward_x.shape, bf16),
            pltpu.VMEM(top.shape, bf16),
            pltpu.VMEM(forward_z[0].shape, bf16),
            pltpu.VMEM(forward_z[1].shape, bf16),
            pltpu.VMEM((groups_x, groups_z, step + groups, LANES), bf16),
            pltpu.VMEM((devices * groups, LANES), f32),
            pltpu.VMEM(((2 * rows + 1) * PADDED, owned * devices), bf16),
            pltpu.VMEM((owned * devices, side), bf16),
            pltpu.VMEM(((2 * rows + 1) * PADDED, side), bf16),
            pltpu.VMEM((2, groups_x, rows, groups, side), f32),
            pltpu.VMEM((2, groups_x, rows, groups, LANES), f32),
            pltpu.VMEM((2 * half_rows, side), bf16),
            pltpu.VMEM((2 * half_rows, width), bf16),
            pltpu.VMEM((2, groups_x, rows, groups, LANES), f32),
            pltpu.VMEM((half_rows, width), f32),
            pltpu.VMEM((2, groups_x, rows, groups, side), f32),
            pltpu.VMEM((rows, LANES, devices), f32),
            pltpu.SemaphoreType.DMA((7,)),
            pltpu.SemaphoreType.DMA((groups_z // 2 + 1,)),
        ],
        compiler_params=pltpu.CompilerParams(vmem_limit_bytes=WHOLE),
        interpret=INTERPRET,
        name="middle",
    )(
        got.reshape(groups_x, groups_z, 2 * step + groups, LANES),
        back_x,
        forward_x,
        top,
        *forward_z,
    )
    got = lax.all_to_all(
        sent.reshape(devices, step + groups, LANES), AXES, 0, 0, tiled=True
    )

    high_term, low_response = pl.pallas_call(
        finish_kernel,
        out_shape=(
            jax.ShapeDtypeStruct((groups, LANES, levels), bf16),
            jax.ShapeDtypeStruct((owned, levels), f32),
        ),
        in_specs=[anywhere] * 2,
        out_specs=(anywhere, pl.BlockSpec(memory_space=pltpu.VMEM)),
        scratch_shapes=[
            pltpu.VMEM((devices, step + groups, LANES), bf16),
            pltpu.VMEM((owned, levels, levels), bf16),
            pltpu.VMEM((LANES * groups, LANES), f32),
            pltpu.VMEM((devices * groups, LANES), f32),
            pltpu.VMEM((levels, LANES), f32),
            pltpu.VMEM((groups, LANES, levels), bf16),
            pltpu.SemaphoreType.DMA((devices * rows // LANES,)),
            pltpu.SemaphoreType.DMA((owned,)),
            pltpu.SemaphoreType.DMA((devices * rows // LANES,)),
        ],
        compiler_params=pltpu.CompilerParams(vmem_limit_bytes=WHOLE),
        interpret=INTERPRET,
        name="finish",
    )(got, tau_inverse)
    return (high_term.reshape(cells_x, cells_z, levels), low_response)


def solution(mesh):
    placed = (
        P("gx", "gz", None),
        P("gx", "gz", None),
        P(AXES, None),
        P(AXES, None),
        P(AXES),
        P(AXES),
        P(AXES, None, None),
    )
    return jax.shard_map(
        on_device,
        mesh=mesh,
        in_specs=placed,
        out_specs=(P("gx", "gz", None), P(AXES, None)),
        check_vma=False,
    )
```

```python
import functools
import math

import jax
import jax.numpy as jnp
from jax import lax
from jax.experimental import pallas as pl
from jax.experimental.pallas import tpu as pltpu
from jax.sharding import PartitionSpec as P

KL = 32
SIDE = 2 * KL + 1
PADDED = 80
LANES = 128
HALF = LANES // 2
AXES = ("gx", "gz")
INTERPRET = False
WHOLE = 67043328
bf16 = jnp.bfloat16
f32 = jnp.float32


def axis_table(index, positions, length):
    wavenum = jnp.where(index <= KL, index, index - KL)
    phases = wavenum[:, None] * positions[None, :] % length
    angles = phases.astype(f32) * (2.0 * math.pi / length)
    return jnp.where((index <= KL)[:, None], jnp.cos(angles), jnp.sin(angles))


def split(values):
    top = lax.reduce_precision(values, 8, 7)
    return top.astype(bf16), (values - top).astype(bf16)


def halves(values):
    top = values.astype(bf16)
    return top, (values - top.astype(f32)).astype(bf16)


def dot(a, b):
    return jnp.dot(a, b, preferred_element_type=f32)


def x_tables(groups_x, groups, group, length_x):
    part = jnp.arange(group, dtype=jnp.int32)[:, None, None]
    device = jnp.arange(groups_x, dtype=jnp.int32)[None, :, None]
    block = jnp.arange(groups, dtype=jnp.int32)[None, None, :]
    where_x = (device * (group * groups) + block * group + part).reshape(-1)
    index = jnp.arange(PADDED, dtype=jnp.int32)
    table = axis_table(index, where_x, length_x)
    table = jnp.where((index < SIDE)[:, None], table, 0.0)
    top, rest = split(table)
    forward = jnp.concatenate([top, rest], axis=0)
    top, rest = split(table.T)
    return forward, jnp.concatenate([top, rest], axis=1)


def z_tables(group, cells_z, length_z):
    column = jnp.arange(length_z * group, dtype=jnp.int32)
    where_z = column // (group * cells_z) * cells_z + column % cells_z
    owner = column // cells_z % group
    index = jnp.arange(1, SIDE, dtype=jnp.int32)
    table = axis_table(index, where_z, length_z)
    part = jnp.arange(group, dtype=jnp.int32)
    inverse = jnp.where(part[:, None, None] == owner[None, None, :], table[None], 0.0)
    inverse = inverse.reshape(group * HALF, -1)
    forward = jnp.where(
        part[None, :, None] == owner[:, None, None], table.T[:, None, :], 0.0
    )
    forward = forward.reshape(-1, group * HALF)
    return inverse.astype(bf16), split(forward)


def across(eye, block):
    return lax.dot_general(
        eye, block, (((1,), (1,)), ((), ())), preferred_element_type=f32
    )


def identity(size):
    return (
        lax.broadcasted_iota(jnp.int32, (size, size), 0)
        == lax.broadcasted_iota(jnp.int32, (size, size), 1)
    ).astype(bf16)


def prepare_kernel(
    u_ref,
    v_ref,
    low_u_ref,
    low_v_ref,
    kx_ref,
    kz_ref,
    out_ref,
    fine,
    lows,
    index,
    tall,
    low,
    tile,
    ready,
    fine_sem,
    low_sem,
    index_sem,
    out_sem,
):
    groups, _, levels = u_ref.shape
    owned = low_u_ref.shape[0]
    devices = out_ref.shape[0]
    rows = levels // devices
    step = rows * groups
    side = 2 * LANES
    pairs = groups // 2
    copies = []
    for k, ref in enumerate((kx_ref, kz_ref)):
        copies.append(pltpu.make_async_copy(ref, index.at[k], index_sem.at[k]))
    for k, ref in enumerate((low_u_ref, low_v_ref)):
        copies.append(pltpu.make_async_copy(ref, lows.at[k], low_sem.at[k]))
    for k, ref in enumerate((u_ref, v_ref)):
        for g in range(pairs):
            at = pl.ds(2 * g, 2)
            copies.append(
                pltpu.make_async_copy(ref.at[at], fine.at[k, at], fine_sem.at[k, g])
            )
    for copy in copies:
        copy.start()
    for copy in copies[:4]:
        copy.wait()

    def send(k, first, count):
        part = (slice(None), pl.ds(first, count))
        return pltpu.make_async_copy(ready.at[part], out_ref.at[part], out_sem.at[k])

    lane = lax.broadcasted_iota(jnp.int32, (1, LANES), 1)

    def place(m, line):
        line = jnp.where(lane == owned + m, index[0, m].astype(f32), line)
        return jnp.where(lane == 2 * owned + m, index[1, m].astype(f32), line)

    line = lax.fori_loop(0, owned, place, jnp.zeros((1, LANES), f32))

    def lower(k, _):
        padded = jnp.concatenate(
            [lows[k].astype(f32), jnp.zeros((LANES - owned, levels), f32)], axis=0
        ).astype(bf16)
        low[...] = jnp.concatenate(
            [
                across(identity(LANES), padded[:, y : y + LANES])
                for y in range(0, levels, LANES)
            ],
            axis=0,
        )
        for y in range(rows):
            tile[pl.ds(k * rows + y, devices, stride=groups), :] = (
                low[pl.ds(y, devices, stride=rows), :] + line
            )
        return 0

    lax.fori_loop(0, 2, lower, 0)
    block = 16

    def round_tile(b, _):
        at = pl.ds(pl.multiple_of(b * block * groups, block * groups), block * groups)
        ready[pl.ds(b * block, block), 2 * step :, :] = (
            tile[at, :].astype(bf16).reshape(block, groups, LANES)
        )
        return 0

    lax.fori_loop(0, devices // block, round_tile, 0)
    send(2, 2 * step, groups).start()

    def turn(k, _):
        def turn_pair(g, _):
            pltpu.make_async_copy(
                u_ref.at[pl.ds(0, 2)], fine.at[k, pl.ds(2 * g, 2)], fine_sem.at[k, g]
            ).wait()
            part = fine[k, pl.ds(2 * g, 2)].reshape(side, levels)
            for y in range(0, levels, side):
                turned = across(identity(side), part[:, y : y + side])
                at = y * groups + 2 * g
                tall[pl.ds(at, side, stride=groups), :] = turned[:, :LANES]
                tall[pl.ds(at + 1, side, stride=groups), :] = turned[:, LANES:]
            return 0

        lax.fori_loop(0, pairs, turn_pair, 0)
        first = pl.multiple_of(k * step, step)

        def round_lines(b, _):
            at = pl.ds(pl.multiple_of(b * block * step, block * step), block * step)
            ready[pl.ds(b * block, block), pl.ds(first, step), :] = (
                tall[at, :].astype(bf16).reshape(block, step, LANES)
            )
            return 0

        lax.fori_loop(0, devices // block, round_lines, 0)
        send(k, first, step).start()
        return 0

    lax.fori_loop(0, 2, turn, 0)
    send(2, 2 * step, groups).wait()
    for k in range(2):
        send(k, k * step, step).wait()


def middle_kernel(
    unitary,
    got_hbm,
    back_x_hbm,
    x_hbm,
    top_hbm,
    z_top_hbm,
    z_rest_hbm,
    out_hbm,
    got_ref,
    back_x_ref,
    x_ref,
    top_ref,
    z_top_ref,
    z_rest_ref,
    out_ref,
    modes,
    turned,
    left,
    right,
    hits,
    table,
    spectrum,
    wave,
    mean,
    wave_top,
    sums,
    cross,
    coefficients,
    force,
    picked,
    in_sem,
    out_sem,
):
    groups_x, groups_z, _, _ = got_ref.shape
    groups = 8
    rows = 4
    owned = 16
    devices = groups_x * groups_z
    step = rows * groups
    points = groups_x * groups
    side = 2 * LANES
    half_rows = groups_x * step
    lane = lax.broadcasted_iota(jnp.int32, (1, LANES), 1)
    low_half = lane < HALF
    which = lane // (LANES // 4)

    everything = (slice(None), slice(None))
    tiles = everything + (pl.ds(2 * step, groups),)
    lines = everything + (pl.ds(0, 2 * step),)
    fetches = [
        pltpu.make_async_copy(source, target, in_sem.at[k])
        for k, (source, target) in enumerate(
            (
                (got_hbm.at[tiles], got_ref.at[tiles]),
                (back_x_hbm, back_x_ref),
                (top_hbm, top_ref),
                (got_hbm.at[lines], got_ref.at[lines]),
                (x_hbm, x_ref),
                (z_top_hbm, z_top_ref),
                (z_rest_hbm, z_rest_ref),
            )
        )
    ]
    for fetch in fetches:
        fetch.start()
    fetches[0].wait()
    def widen(i, _):
        at = pl.ds(pl.multiple_of(i * LANES, LANES), LANES)
        modes[at, :] = got_ref[i, :, 2 * step :, :].astype(f32).reshape(LANES, LANES)
        return 0

    lax.fori_loop(0, groups_x, widen, 0)

    def turn(c, _):
        turned[c] = modes[pl.ds(c, devices, stride=groups), :].T
        return 0

    lax.fori_loop(0, 2 * rows, turn, 0)
    row = lax.broadcasted_iota(jnp.int32, (PADDED, devices), 0).astype(f32)
    wanted = lax.broadcasted_iota(jnp.int32, (LANES, devices), 0)
    wanted = (1 + wanted % HALF).astype(f32)
    table[...] = jnp.zeros_like(table)

    def gather(p, _):
        for e in range(2):
            m = 2 * p + e
            at = slice(e * devices, (e + 1) * devices)
            hit = row == turned[0, pl.ds(owned + m, 1), :]
            hit = jnp.where(hit, 1.0, 0.0).astype(bf16)
            for c in range(2 * rows):
                value = jnp.broadcast_to(turned[c, pl.ds(m, 1), :], (16, devices))
                value = jnp.concatenate([value.astype(bf16)] * (PADDED // 16), axis=0)
                left[c * PADDED : (c + 1) * PADDED, at] = hit * value
            left[2 * rows * PADDED :, at] = hit
            hits[:, pl.ds(pl.multiple_of(m * devices, devices), devices)] = hit
            index_z = turned[0, pl.ds(2 * owned + m, 1), :]
            right[:LANES, at] = jnp.where(wanted == index_z, 1.0, 0.0).astype(bf16)
            right[LANES:, at] = jnp.broadcast_to(
                jnp.where(index_z == 0.0, 1.0, 0.0), (LANES, devices)
            ).astype(bf16)
        table[...] += across(left[...], right[...])
        return 0

    lax.fori_loop(0, owned // 2, gather, 0)

    def round_table(c, _):
        at = pl.ds(pl.multiple_of(c * PADDED, PADDED), PADDED)
        spectrum[at, :] = table[at, :].astype(bf16)
        return 0

    lax.fori_loop(0, 2 * rows + 1, round_table, 0)
    fetches[1].wait()

    def spread(k, y, part):
        full = dot(back_x_ref[...], jnp.concatenate([part, part], axis=0))
        part = [full[p * points : (p + 1) * points] for p in range(4)]
        waves = jnp.concatenate(
            [
                jnp.where(low_half, part[0][:, :LANES], part[1][:, :LANES]),
                jnp.where(low_half, part[2][:, :LANES], part[3][:, :LANES]),
            ],
            axis=1,
        )
        constant = part[3][:, LANES:]
        for p in range(3):
            constant = jnp.where(which == p, part[p][:, LANES:], constant)
        wave[k, :, y] = waves.reshape(groups_x, groups, side)
        mean[k, :, y] = constant.reshape(groups_x, groups, LANES)

    def spread_low(c, _):
        at = pl.ds(pl.multiple_of(c * PADDED, PADDED), PADDED)
        spread(c // rows, c % rows, spectrum[at, :])
        return 0

    lax.fori_loop(0, 2 * rows, spread_low, 0)

    def round_wave(k, _):
        at = pl.ds(pl.multiple_of(k * half_rows, half_rows), half_rows)
        wave_top[at, :] = wave[k].reshape(half_rows, side).astype(bf16)
        return 0

    lax.fori_loop(0, 2, round_wave, 0)
    sums[...] = jnp.zeros_like(sums)
    coefficients[...] = jnp.zeros_like(coefficients)
    for fetch in fetches[2:]:
        fetch.wait()

    def fine(j, k):
        parts = [
            got_ref[:, 2 * j + e, k * step : (k + 1) * step, :].reshape(half_rows, LANES)
            for e in range(2)
        ]
        return jnp.concatenate(parts, axis=1).astype(f32)

    def multiply(j, _):
        at = pl.ds(pl.multiple_of(j * side, side), side)
        coarse = dot(wave_top[...], top_ref[:, at])
        flat = mean[...].reshape(2 * half_rows, LANES)
        coarse = coarse + jnp.concatenate([flat, flat], axis=1)
        coarse_u, coarse_v = coarse[:half_rows], coarse[half_rows:]
        fine_u, fine_v = fine(j, 0), fine(j, 1)
        self_term = (coarse_u * coarse_v + fine_u * fine_v).astype(bf16)
        cross_term = coarse_u * fine_v + fine_u * coarse_v
        cross[:, at] = cross_term
        cross_round = cross_term.astype(bf16)
        for k, term in enumerate((self_term, cross_round)):
            wide = term.astype(f32)
            sums[k] += (wide[:, :LANES] + wide[:, LANES:]).reshape(
                groups_x, rows, groups, LANES
            )
            share = dot(term, z_top_ref[at, :]) + dot(term, z_rest_ref[at, :])
            coefficients[k] += share.reshape(groups_x, rows, groups, side)
        return 0

    lax.fori_loop(0, groups_z // 2, multiply, 0)

    def project(k, y):
        waves = coefficients[k, :, y].reshape(points, side)
        total = sums[k, :, y].reshape(points, LANES)
        stack = []
        for part in range(4):
            half = waves[:, :LANES] if part < 2 else waves[:, LANES:]
            keep = low_half if part % 2 == 0 else jnp.logical_not(low_half)
            stack.append(
                jnp.concatenate(
                    [
                        jnp.where(keep, half, 0.0),
                        jnp.where(which == part, total, 0.0),
                    ],
                    axis=1,
                )
            )
        top, rest = halves(jnp.concatenate(stack, axis=0))
        outer = dot(x_ref[...], top)
        outer = outer[:PADDED] + outer[PADDED:] + dot(x_ref[:PADDED], rest)
        waves = outer[:, :LANES] * unitary
        waves = waves + pltpu.roll(waves, HALF, 1)
        constant = jnp.sum(outer[:, LANES:], axis=1, keepdims=True) * unitary
        return waves, jnp.broadcast_to(constant, (PADDED, LANES))

    row_index = lax.broadcasted_iota(jnp.int32, (PADDED, 1), 0)
    weight_x = jnp.where(row_index > 0, 2.0, 1.0).astype(f32)

    def restore(y, _):
        waves, constant = project(1, y)
        low = jnp.concatenate([waves * (2.0 * weight_x), constant * weight_x], axis=1)
        spread(0, y, low.astype(bf16) * spectrum[2 * rows * PADDED :, :])
        return 0

    lax.fori_loop(0, rows, restore, 0)
    lax.fori_loop(0, 1, round_wave, 0)

    def push(y, _):
        waves, constant = project(0, y)
        value = jnp.where(low_half, waves, jnp.where(lane == HALF, constant, 0.0))
        value = jnp.concatenate([value, jnp.zeros((LANES - PADDED, LANES), f32)], axis=0)
        force[y] = value.T[:PADDED]
        return 0

    lax.fori_loop(0, rows, push, 0)
    line = lax.broadcasted_iota(jnp.int32, (PADDED, devices), 0)
    line = jnp.where(line < HALF, line + 1, jnp.where(line == HALF, 0, -1)).astype(f32)
    picked[...] = jnp.zeros_like(picked)

    def pick(p, _):
        at = pl.ds(pl.multiple_of(p * 2 * devices, 2 * devices), 2 * devices)
        values = force[...].reshape(rows * PADDED, LANES).astype(bf16)[:, :PADDED]
        chosen = dot(values, hits[:, at])
        for e in range(2):
            m = 2 * p + e
            hit = line == turned[0, pl.ds(2 * owned + m, 1), :]
            for y in range(rows):
                value = chosen[
                    y * PADDED : (y + 1) * PADDED, e * devices : (e + 1) * devices
                ]
                picked[y, pl.ds(m, 1), :] = jnp.sum(
                    jnp.where(hit, value, 0.0), axis=0, keepdims=True
                )
        return 0

    lax.fori_loop(0, owned // 2, pick, 0)
    modes[...] = jnp.zeros_like(modes)

    def turn_back(y, _):
        modes[pl.ds(y, devices, stride=groups), :] = picked[y].T
        return 0

    lax.fori_loop(0, rows, turn_back, 0)

    def narrow(i, _):
        at = pl.ds(pl.multiple_of(i * LANES, LANES), LANES)
        out_ref[i, :, step:, :] = modes[at, :].astype(bf16).reshape(
            groups_z, groups, LANES
        )
        return 0

    lax.fori_loop(0, groups_x, narrow, 0)
    part = everything + (pl.ds(step, groups),)
    send_tiles = pltpu.make_async_copy(
        out_ref.at[part], out_hbm.at[part], out_sem.at[groups_z // 2]
    )
    send_tiles.start()

    def send(j):
        part = (slice(None), pl.ds(2 * j, 2), pl.ds(0, step))
        return pltpu.make_async_copy(out_ref.at[part], out_hbm.at[part], out_sem.at[j])

    def subtract(j, _):
        at = pl.ds(pl.multiple_of(j * side, side), side)
        restored = dot(wave_top[:half_rows], top_ref[:, at])
        flat = mean[0].reshape(half_rows, LANES)
        restored = restored + jnp.concatenate([flat, flat], axis=1)
        high = (cross[:, at] - unitary * restored).astype(bf16)
        for e in range(2):
            out_ref[:, 2 * j + e, :step, :] = high[:, e * LANES : (e + 1) * LANES].reshape(
                groups_x, step, LANES
            )
        send(j).start()
        return 0

    lax.fori_loop(0, groups_z // 2, subtract, 0)
    send_tiles.wait()

    def drain(j, _):
        send(j).wait()
        return 0

    lax.fori_loop(0, groups_z // 2, drain, 0)


def finish_kernel(
    got_hbm,
    tau_hbm,
    high_hbm,
    low_ref,
    got_ref,
    tau_ref,
    tall,
    tile,
    force,
    vector,
    ready,
    got_sem,
    tau_sem,
    out_sem,
):
    devices = got_hbm.shape[0]
    owned, levels, _ = tau_hbm.shape
    rows = levels // devices
    groups = high_hbm.shape[0]
    step = rows * groups
    chunk = LANES // rows
    count = devices // chunk
    fetches = []
    for q in range(count):
        at = pl.ds(q * chunk, chunk)
        fetches.append(
            pltpu.make_async_copy(got_hbm.at[at], got_ref.at[at], got_sem.at[q])
        )
    for m in range(owned):
        fetches.append(
            pltpu.make_async_copy(tau_hbm.at[m], tau_ref.at[m], tau_sem.at[m])
        )
    for fetch in fetches:
        fetch.start()
    def send(q):
        part = (slice(None), slice(None), pl.ds(pl.multiple_of(q * LANES, LANES), LANES))
        return pltpu.make_async_copy(ready.at[part], high_hbm.at[part], out_sem.at[q])

    def turn(q, _):
        at = pl.ds(q * chunk, chunk)
        pltpu.make_async_copy(got_hbm.at[at], got_ref.at[at], got_sem.at[q]).wait()
        tall[...] = got_ref[at, :step, :].astype(f32).reshape(chunk * step, LANES)
        where = pl.ds(pl.multiple_of(q * LANES, LANES), LANES)
        for g in range(groups):
            column = tall[pl.ds(g, LANES, stride=groups), :].astype(bf16)
            ready[g, :, where] = across(identity(LANES), column).astype(bf16)
        send(q).start()
        return 0

    lax.fori_loop(0, count, turn, 0)
    tile[...] = got_ref[:, step:, :].astype(f32).reshape(devices * groups, LANES)
    for y in range(rows):
        force[pl.ds(y, devices, stride=rows), :] = tile[
            pl.ds(y, devices, stride=groups), :
        ]
    vector[...] = force[...].astype(bf16)
    lane = lax.broadcasted_iota(jnp.int32, (1, LANES), 1)

    def solve(m, _):
        pltpu.make_async_copy(tau_hbm.at[m], tau_ref.at[m], tau_sem.at[m]).wait()
        force[...] = jnp.where(lane == m, dot(tau_ref[m], vector[...]), force[...])
        return 0

    lax.fori_loop(0, owned, solve, 0)
    low_ref[...] = force[...].T[:owned]

    def drain(q, _):
        send(q).wait()
        return 0

    lax.fori_loop(0, count, drain, 0)


def on_device(high_u, high_v, low_u, low_v, low_kx, low_kz, tau_inverse):
    cells_x, cells_z, levels = high_u.shape
    owned = low_u.shape[0]
    groups_x = lax.axis_size("gx")
    groups_z = lax.axis_size("gz")
    devices = groups_x * groups_z
    length_x = groups_x * cells_x
    length_z = groups_z * cells_z
    rows = levels // devices
    group = LANES // cells_z
    groups = cells_x // group
    step = rows * groups
    points = groups_x * groups
    half_rows = groups_x * step
    width = groups_z * LANES
    side = 2 * LANES
    unitary = 1.0 / math.sqrt(length_x * length_z)

    anywhere = pl.BlockSpec(memory_space=pltpu.HBM)
    sent = pl.pallas_call(
        prepare_kernel,
        out_shape=jax.ShapeDtypeStruct((devices, 2 * step + groups, LANES), bf16),
        in_specs=[anywhere] * 6,
        out_specs=anywhere,
        scratch_shapes=[
            pltpu.VMEM((2, groups, LANES, levels), bf16),
            pltpu.VMEM((2, owned, levels), bf16),
            pltpu.SMEM((2, owned), jnp.int32),
            pltpu.VMEM((levels * groups, LANES), f32),
            pltpu.VMEM((levels, LANES), f32),
            pltpu.VMEM((devices * groups, LANES), f32),
            pltpu.VMEM((devices, 2 * step + groups, LANES), bf16),
            pltpu.SemaphoreType.DMA((2, groups // 2)),
            pltpu.SemaphoreType.DMA((2,)),
            pltpu.SemaphoreType.DMA((2,)),
            pltpu.SemaphoreType.DMA((3,)),
        ],
        compiler_params=pltpu.CompilerParams(vmem_limit_bytes=WHOLE),
        interpret=INTERPRET,
        name="prepare",
    )(
        high_u.reshape(groups, LANES, levels),
        high_v.reshape(groups, LANES, levels),
        low_u,
        low_v,
        low_kx,
        low_kz,
    )
    got = lax.all_to_all(sent, AXES, 0, 0, tiled=True)

    forward_x, back_x = x_tables(groups_x, groups, group, length_x)
    top, forward_z = z_tables(group, cells_z, length_z)
    sent = pl.pallas_call(
        functools.partial(middle_kernel, unitary),
        out_shape=jax.ShapeDtypeStruct((groups_x, groups_z, step + groups, LANES), bf16),
        in_specs=[anywhere] * 6,
        out_specs=anywhere,
        scratch_shapes=[
            pltpu.VMEM((groups_x, groups_z, 2 * step + groups, LANES), bf16),
            pltpu.VMEM(back_x.shape, bf16),
            pltpu.VMEM(forward_x.shape, bf16),
            pltpu.VMEM(top.shape, bf16),
            pltpu.VMEM(forward_z[0].shape, bf16),
            pltpu.VMEM(forward_z[1].shape, bf16),
            pltpu.VMEM((groups_x, groups_z, step + groups, LANES), bf16),
            pltpu.VMEM((devices * groups, LANES), f32),
            pltpu.VMEM((2 * rows, LANES, devices), f32),
            pltpu.VMEM(((2 * rows + 1) * PADDED, 2 * devices), bf16),
            pltpu.VMEM((side, 2 * devices), bf16),
            pltpu.VMEM((PADDED, owned * devices), bf16),
            pltpu.VMEM(((2 * rows + 1) * PADDED, side), f32),
            pltpu.VMEM(((2 * rows + 1) * PADDED, side), bf16),
            pltpu.VMEM((2, groups_x, rows, groups, side), f32),
            pltpu.VMEM((2, groups_x, rows, groups, LANES), f32),
            pltpu.VMEM((2 * half_rows, side), bf16),
            pltpu.VMEM((2, groups_x, rows, groups, LANES), f32),
            pltpu.VMEM((half_rows, width), f32),
            pltpu.VMEM((2, groups_x, rows, groups, side), f32),
            pltpu.VMEM((rows, PADDED, LANES), f32),
            pltpu.VMEM((rows, LANES, devices), f32),
            pltpu.SemaphoreType.DMA((7,)),
            pltpu.SemaphoreType.DMA((groups_z // 2 + 1,)),
        ],
        compiler_params=pltpu.CompilerParams(vmem_limit_bytes=WHOLE),
        interpret=INTERPRET,
        name="middle",
    )(
        got.reshape(groups_x, groups_z, 2 * step + groups, LANES),
        back_x,
        forward_x,
        top,
        *forward_z,
    )
    got = lax.all_to_all(
        sent.reshape(devices, step + groups, LANES), AXES, 0, 0, tiled=True
    )

    high_term, low_response = pl.pallas_call(
        finish_kernel,
        out_shape=(
            jax.ShapeDtypeStruct((groups, LANES, levels), bf16),
            jax.ShapeDtypeStruct((owned, levels), f32),
        ),
        in_specs=[anywhere] * 2,
        out_specs=(anywhere, pl.BlockSpec(memory_space=pltpu.VMEM)),
        scratch_shapes=[
            pltpu.VMEM((devices, step + groups, LANES), bf16),
            pltpu.VMEM((owned, levels, levels), bf16),
            pltpu.VMEM((LANES * groups, LANES), f32),
            pltpu.VMEM((devices * groups, LANES), f32),
            pltpu.VMEM((levels, LANES), f32),
            pltpu.VMEM((levels, LANES), bf16),
            pltpu.VMEM((groups, LANES, levels), bf16),
            pltpu.SemaphoreType.DMA((devices * rows // LANES,)),
            pltpu.SemaphoreType.DMA((owned,)),
            pltpu.SemaphoreType.DMA((devices * rows // LANES,)),
        ],
        compiler_params=pltpu.CompilerParams(vmem_limit_bytes=WHOLE),
        interpret=INTERPRET,
        name="finish",
    )(got, tau_inverse)
    return (high_term.reshape(cells_x, cells_z, levels), low_response)


def solution(mesh):
    placed = (
        P("gx", "gz", None),
        P("gx", "gz", None),
        P(AXES, None),
        P(AXES, None),
        P(AXES),
        P(AXES),
        P(AXES, None, None),
    )
    return jax.shard_map(
        on_device,
        mesh=mesh,
        in_specs=placed,
        out_specs=(P("gx", "gz", None), P(AXES, None)),
        check_vma=False,
    )
```

```python
import functools
import math

import jax
import jax.numpy as jnp
from jax import lax
from jax.experimental import pallas as pl
from jax.experimental.pallas import tpu as pltpu
from jax.sharding import PartitionSpec as P

KL = 32
SIDE = 2 * KL + 1
PADDED = 80
LANES = 128
HALF = LANES // 2
AXES = ("gx", "gz")
INTERPRET = False
MIB = 1024 * 1024
WHOLE = 67043328
PREPARE = WHOLE
MIDDLE = 24 * MIB
STAGE = 16 * MIB
FINISH = 16 * MIB
bf16 = jnp.bfloat16
f32 = jnp.float32


def axis_table(index, positions, length):
    wavenum = jnp.where(index <= KL, index, index - KL)
    phases = wavenum[:, None] * positions[None, :] % length
    angles = phases.astype(f32) * (2.0 * math.pi / length)
    return jnp.where((index <= KL)[:, None], jnp.cos(angles), jnp.sin(angles))


def split(values):
    top = lax.reduce_precision(values, 8, 7)
    return top.astype(bf16), (values - top).astype(bf16)


def halves(values):
    top = values.astype(bf16)
    return top, (values - top.astype(f32)).astype(bf16)


def dot(a, b):
    return jnp.dot(a, b, preferred_element_type=f32)


def x_tables(groups_x, groups, group, length_x):
    part = jnp.arange(group, dtype=jnp.int32)[:, None, None]
    device = jnp.arange(groups_x, dtype=jnp.int32)[None, :, None]
    block = jnp.arange(groups, dtype=jnp.int32)[None, None, :]
    where_x = (device * (group * groups) + block * group + part).reshape(-1)
    index = jnp.arange(PADDED, dtype=jnp.int32)
    table = axis_table(index, where_x, length_x)
    table = jnp.where((index < SIDE)[:, None], table, 0.0)
    top, rest = split(table)
    forward = jnp.concatenate([top, rest], axis=0)
    top, rest = split(table.T)
    return forward, jnp.concatenate([top, rest], axis=1)


def z_tables(group, cells_z, length_z):
    column = jnp.arange(length_z * group, dtype=jnp.int32)
    where_z = column // (group * cells_z) * cells_z + column % cells_z
    owner = column // cells_z % group
    index = jnp.arange(1, SIDE, dtype=jnp.int32)
    table = axis_table(index, where_z, length_z)
    part = jnp.arange(group, dtype=jnp.int32)
    forward = jnp.where(
        part[None, :, None] == owner[:, None, None], table.T[:, None, :], 0.0
    )
    return split(forward.reshape(-1, group * HALF))


def across(eye, block):
    return lax.dot_general(
        eye, block, (((1,), (1,)), ((), ())), preferred_element_type=f32
    )


def identity(size):
    return (
        lax.broadcasted_iota(jnp.int32, (size, size), 0)
        == lax.broadcasted_iota(jnp.int32, (size, size), 1)
    ).astype(bf16)


def prepare_kernel(
    u_ref,
    v_ref,
    low_u_ref,
    low_v_ref,
    kx_ref,
    kz_ref,
    out_ref,
    fine,
    lows,
    index,
    tall,
    low,
    tile,
    ready,
    fine_sem,
    low_sem,
    index_sem,
    out_sem,
):
    groups, _, levels = u_ref.shape
    owned = low_u_ref.shape[0]
    devices = out_ref.shape[0]
    rows = levels // devices
    step = rows * groups
    side = 2 * LANES
    pairs = groups // 2
    copies = []
    for k, ref in enumerate((kx_ref, kz_ref)):
        copies.append(pltpu.make_async_copy(ref, index.at[k], index_sem.at[k]))
    for k, ref in enumerate((low_u_ref, low_v_ref)):
        copies.append(pltpu.make_async_copy(ref, lows.at[k], low_sem.at[k]))
    for k, ref in enumerate((u_ref, v_ref)):
        for g in range(pairs):
            at = pl.ds(2 * g, 2)
            copies.append(
                pltpu.make_async_copy(ref.at[at], fine.at[k, at], fine_sem.at[k, g])
            )
    for copy in copies[4 : 4 + pairs] + copies[:4]:
        copy.start()

    def send(k, first, count):
        part = (slice(None), pl.ds(first, count))
        return pltpu.make_async_copy(ready.at[part], out_ref.at[part], out_sem.at[k])

    sends = []
    for k in range(2):
        for g in range(pairs):
            copies[4 + k * pairs + g].wait()
            if k + g == 0:
                for copy in copies[4 + pairs :]:
                    copy.start()
            block = fine[k, 2 * g : 2 * g + 2].reshape(side, levels)
            for y in range(0, levels, side):
                turned = block[:, y : y + side].astype(f32).T
                at = y * groups + 2 * g
                tall[pl.ds(at, side, stride=groups), :] = turned[:, :LANES]
                tall[pl.ds(at + 1, side, stride=groups), :] = turned[:, LANES:]
        ready[:, k * step : (k + 1) * step, :] = (
            tall[...].astype(bf16).reshape(devices, step, LANES)
        )
        sends.append(send(k, k * step, step))
        sends[-1].start()
        if k == 1:
            continue
        for copy in copies[:4]:
            copy.wait()
        lane = lax.broadcasted_iota(jnp.int32, (1, LANES), 1)
        line = jnp.zeros((1, LANES), f32)
        for m in range(owned):
            line = jnp.where(lane == owned + m, index[0, m].astype(f32), line)
            line = jnp.where(lane == 2 * owned + m, index[1, m].astype(f32), line)
        small = identity(LANES)
        for h in range(2):
            padded = jnp.concatenate(
                [lows[h].astype(f32), jnp.zeros((LANES - owned, levels), f32)], axis=0
            ).astype(bf16)
            for y in range(0, levels, LANES):
                low[pl.ds(y, LANES), :] = across(small, padded[:, y : y + LANES])
            for y in range(rows):
                tile[pl.ds(h * rows + y, devices, stride=groups), :] = (
                    low[pl.ds(y, devices, stride=rows), :] + line
                )
        ready[:, 2 * step :, :] = tile[...].astype(bf16).reshape(devices, groups, LANES)
        sends.append(send(2, 2 * step, groups))
        sends[-1].start()
    for copy in sends:
        copy.wait()


def middle_kernel(
    unitary,
    got_ref,
    tables,
    x_ref,
    out_ref,
    modes,
    left,
    right,
    spectrum,
    wave,
    mean,
    wave_top,
    products,
    sums,
    cross,
    coefficients,
    picked,
):
    groups_x, groups_z, _, _ = got_ref.shape
    groups = 8
    rows = 4
    owned = 16
    devices = groups_x * groups_z
    step = rows * groups
    points = groups_x * groups
    side = 2 * LANES
    half_rows = groups_x * step
    lane = lax.broadcasted_iota(jnp.int32, (1, LANES), 1)
    low_half = lane < HALF
    which = lane // (LANES // 4)

    width = groups_z * LANES
    modes[...] = got_ref[:, :, 2 * step :, :].astype(f32).reshape(devices * groups, LANES)
    first = modes[pl.ds(0, devices, stride=groups), :]
    turned = [first.T]
    for c in range(1, 2 * rows):
        turned.append(modes[pl.ds(c, devices, stride=groups), :].T)
    row = lax.broadcasted_iota(jnp.int32, (PADDED, devices), 0).astype(f32)
    column = lax.broadcasted_iota(jnp.int32, (devices, LANES), 1)
    wanted = (1 + column % HALF).astype(f32)
    for m in range(owned):
        at = slice(m * devices, (m + 1) * devices)
        hit = row == turned[0][owned + m : owned + m + 1, :]
        hit = jnp.where(hit, 1.0, 0.0).astype(bf16)
        for c in range(2 * rows):
            value = jnp.broadcast_to(turned[c][m : m + 1, :], (16, devices)).astype(bf16)
            value = jnp.concatenate([value] * (PADDED // 16), axis=0)
            left[c * PADDED : (c + 1) * PADDED, at] = hit * value
        left[2 * rows * PADDED :, at] = hit
        index_z = jnp.broadcast_to(
            first[:, 2 * owned + m : 2 * owned + m + 1], (devices, LANES)
        )
        right[at, :LANES] = jnp.where(wanted == index_z, 1.0, 0.0).astype(bf16)
        right[at, LANES:] = jnp.where(index_z == 0.0, 1.0, 0.0).astype(bf16)
    spectrum[...] = dot(left[...], right[...]).astype(bf16)

    def spread(k, parts):
        both = jnp.concatenate(parts, axis=1)
        back = tables[2 * width :, : 2 * PADDED]
        full = dot(back, jnp.concatenate([both, both], axis=0))
        for y in range(len(parts)):
            part = [
                full[p * points : (p + 1) * points, y * side : (y + 1) * side]
                for p in range(4)
            ]
            waves = jnp.concatenate(
                [
                    jnp.where(low_half, part[0][:, :LANES], part[1][:, :LANES]),
                    jnp.where(low_half, part[2][:, :LANES], part[3][:, :LANES]),
                ],
                axis=1,
            )
            constant = part[3][:, LANES:]
            for p in range(3):
                constant = jnp.where(which == p, part[p][:, LANES:], constant)
            wave[k, :, y] = waves.reshape(groups_x, groups, side)
            mean[k, :, y] = constant.reshape(groups_x, groups, LANES)

    for k in range(2):
        spread(
            k,
            [
                spectrum[(k * rows + y) * PADDED : (k * rows + y + 1) * PADDED, :]
                for y in range(rows)
            ],
        )
    wave_top[...] = wave[...].reshape(2 * half_rows, side).astype(bf16)
    sums[...] = jnp.zeros_like(sums)

    def fine(j, k):
        parts = [
            got_ref[:, 2 * j + e, k * step : (k + 1) * step, :].reshape(half_rows, LANES)
            for e in range(2)
        ]
        return jnp.concatenate(parts, axis=1).astype(f32)

    def multiply(j, _):
        at = pl.ds(pl.multiple_of(j * side, side), side)
        coarse = across(wave_top[...], tables[at, :])
        flat = mean[...].reshape(2 * half_rows, LANES)
        coarse = coarse + jnp.concatenate([flat, flat], axis=1)
        coarse_u, coarse_v = coarse[:half_rows], coarse[half_rows:]
        fine_u, fine_v = fine(j, 0), fine(j, 1)
        self_term = (coarse_u * coarse_v + fine_u * fine_v).astype(bf16)
        cross_term = coarse_u * fine_v + fine_u * coarse_v
        cross[:, at] = cross_term
        cross_round = cross_term.astype(bf16)
        products[:half_rows, at] = self_term
        products[half_rows:, at] = cross_round
        for k, term in enumerate((self_term, cross_round)):
            wide = term.astype(f32)
            sums[k] += (wide[:, :LANES] + wide[:, LANES:]).reshape(
                groups_x, rows, groups, LANES
            )
        return 0

    lax.fori_loop(0, groups_z // 2, multiply, 0, unroll=1)
    both = dot(products[...], tables[:width, :])
    both = both + dot(products[...], tables[width : 2 * width, :])
    coefficients[...] = both.reshape(2, groups_x, rows, groups, side)

    def project(k):
        stacks = []
        for y in range(rows):
            waves = coefficients[k, :, y].reshape(points, side)
            total = sums[k, :, y].reshape(points, LANES)
            stack = []
            for part in range(4):
                half = waves[:, :LANES] if part < 2 else waves[:, LANES:]
                keep = low_half if part % 2 == 0 else jnp.logical_not(low_half)
                stack.append(
                    jnp.concatenate(
                        [
                            jnp.where(keep, half, 0.0),
                            jnp.where(which == part, total, 0.0),
                        ],
                        axis=1,
                    )
                )
            stacks.append(jnp.concatenate(stack, axis=0))
        top, rest = halves(jnp.concatenate(stacks, axis=1))
        table_x = x_ref[...]
        outer = dot(table_x, top)
        outer = outer[:PADDED] + outer[PADDED:] + dot(table_x[:PADDED], rest)
        done = []
        for y in range(rows):
            waves = outer[:, y * side : y * side + LANES] * unitary
            waves = waves + pltpu.roll(waves, HALF, 1)
            constant = outer[:, y * side + LANES : (y + 1) * side]
            constant = jnp.sum(constant, axis=1, keepdims=True) * unitary
            done.append((waves, jnp.broadcast_to(constant, (PADDED, LANES))))
        return done

    row_index = lax.broadcasted_iota(jnp.int32, (PADDED, 1), 0)
    weight_x = jnp.where(row_index > 0, 2.0, 1.0).astype(f32)
    mask = spectrum[2 * rows * PADDED :, :]
    parts = []
    for waves, constant in project(1):
        low = jnp.concatenate([waves * (2.0 * weight_x), constant * weight_x], axis=1)
        parts.append(low.astype(bf16) * mask)
    spread(0, parts)
    wave_top[:half_rows] = wave[0].reshape(half_rows, side).astype(bf16)

    def subtract(j, _):
        at = pl.ds(pl.multiple_of(j * side, side), side)
        restored = across(wave_top[:half_rows], tables[at, :])
        flat = mean[0].reshape(half_rows, LANES)
        restored = restored + jnp.concatenate([flat, flat], axis=1)
        high = (cross[:, at] - unitary * restored).astype(bf16)
        for e in range(2):
            out_ref[:, 2 * j + e, :step, :] = high[:, e * LANES : (e + 1) * LANES].reshape(
                groups_x, step, LANES
            )
        return 0

    lax.fori_loop(0, groups_z // 2, subtract, 0, unroll=1)

    lines = 72
    parts = []
    for waves, constant in project(0):
        force = jnp.where(low_half, waves, jnp.where(lane == HALF, constant, 0.0))
        force = jnp.concatenate([force, jnp.zeros((LANES - PADDED, LANES), f32)], axis=0)
        parts.append(force.T[:lines])
    force = jnp.concatenate(parts, axis=0).astype(bf16)[:, :PADDED]
    line = lax.broadcasted_iota(jnp.int32, (lines, devices), 0)
    line = jnp.where(line < HALF, line + 1, jnp.where(line == HALF, 0, -1)).astype(f32)
    picked[...] = jnp.zeros_like(picked)
    for m in range(0, owned, 2):
        chosen = dot(force, left[2 * rows * PADDED :, m * devices : (m + 2) * devices])
        for e in range(2):
            hit = line == turned[0][2 * owned + m + e : 2 * owned + m + e + 1, :]
            for y in range(rows):
                value = chosen[y * lines : (y + 1) * lines, e * devices : (e + 1) * devices]
                picked[y, m + e : m + e + 1, :] = jnp.sum(
                    jnp.where(hit, value, 0.0), axis=0, keepdims=True
                )
    modes[...] = jnp.zeros_like(modes)
    for y in range(rows):
        modes[pl.ds(y, devices, stride=groups), :] = picked[y].T
    out_ref[:, :, step:, :] = (
        modes[...].astype(bf16).reshape(groups_x, groups_z, groups, LANES)
    )


def finish_kernel(got_ref, tau_ref, high_hbm, low_ref, tall, tile, force, ready, out_sem):
    devices = got_ref.shape[0]
    owned, levels, _ = tau_ref.shape
    rows = levels // devices
    groups = high_hbm.shape[0]
    step = rows * groups
    chunk = LANES // rows
    sends = []
    for q in range(devices // chunk):
        at = slice(q * chunk, (q + 1) * chunk)
        tall[...] = got_ref[at, :step, :].astype(f32).reshape(chunk * step, LANES)
        where = slice(q * LANES, (q + 1) * LANES)
        for g in range(groups):
            column = tall[pl.ds(g, LANES, stride=groups), :]
            ready[g, :, where] = column.T.astype(bf16)
        part = (slice(None), slice(None), pl.ds(q * LANES, LANES))
        sends.append(
            pltpu.make_async_copy(ready.at[part], high_hbm.at[part], out_sem.at[q])
        )
        sends[-1].start()
    tile[...] = got_ref[:, step:, :].astype(f32).reshape(devices * groups, LANES)
    for y in range(rows):
        force[pl.ds(y, devices, stride=rows), :] = tile[
            pl.ds(y, devices, stride=groups), :
        ]
    vector = force[...].astype(bf16)
    lane = lax.broadcasted_iota(jnp.int32, (1, LANES), 1)
    answer = jnp.zeros((levels, LANES), f32)
    for m in range(owned):
        answer = jnp.where(lane == m, dot(tau_ref[m], vector), answer)
    low_ref[...] = answer.T[:owned]
    for copy in sends:
        copy.wait()


def stage_kernel(*refs):
    count = (len(refs) - 1) // 2
    copies = [
        pltpu.make_async_copy(refs[k], refs[count + k], refs[-1].at[k])
        for k in range(count)
    ]
    for copy in copies:
        copy.start()
    for copy in copies:
        copy.wait()


def on_device(high_u, high_v, low_u, low_v, low_kx, low_kz, tau_inverse):
    cells_x, cells_z, levels = high_u.shape
    owned = low_u.shape[0]
    groups_x = lax.axis_size("gx")
    groups_z = lax.axis_size("gz")
    devices = groups_x * groups_z
    length_x = groups_x * cells_x
    length_z = groups_z * cells_z
    rows = levels // devices
    group = LANES // cells_z
    groups = cells_x // group
    step = rows * groups
    points = groups_x * groups
    half_rows = groups_x * step
    width = groups_z * LANES
    side = 2 * LANES
    unitary = 1.0 / math.sqrt(length_x * length_z)

    anywhere = pl.BlockSpec(memory_space=pltpu.HBM)
    near = pl.BlockSpec(memory_space=pltpu.VMEM)
    sent = pl.pallas_call(
        prepare_kernel,
        out_shape=jax.ShapeDtypeStruct((devices, 2 * step + groups, LANES), bf16),
        in_specs=[anywhere] * 6,
        out_specs=anywhere,
        scratch_shapes=[
            pltpu.VMEM((2, groups, LANES, levels), bf16),
            pltpu.VMEM((2, owned, levels), bf16),
            pltpu.SMEM((2, owned), jnp.int32),
            pltpu.VMEM((levels * groups, LANES), f32),
            pltpu.VMEM((levels, LANES), f32),
            pltpu.VMEM((devices * groups, LANES), f32),
            pltpu.VMEM((devices, 2 * step + groups, LANES), bf16),
            pltpu.SemaphoreType.DMA((2, groups // 2)),
            pltpu.SemaphoreType.DMA((2,)),
            pltpu.SemaphoreType.DMA((2,)),
            pltpu.SemaphoreType.DMA((3,)),
        ],
        compiler_params=pltpu.CompilerParams(vmem_limit_bytes=PREPARE),
        interpret=INTERPRET,
        name="prepare",
    )(
        high_u.reshape(groups, LANES, levels),
        high_v.reshape(groups, LANES, levels),
        low_u,
        low_v,
        low_kx,
        low_kz,
    )
    got = lax.all_to_all(sent, AXES, 0, 0, tiled=True)

    forward_x, back_x = x_tables(groups_x, groups, group, length_x)
    back_x = jnp.pad(back_x, ((0, 0), (0, side - 2 * PADDED)))
    tables = jnp.concatenate([*z_tables(group, cells_z, length_z), back_x], axis=0)
    kept = (tau_inverse, forward_x)
    tau_inverse, staged_x = pl.pallas_call(
        stage_kernel,
        out_shape=[jax.ShapeDtypeStruct(a.shape, a.dtype) for a in kept],
        in_specs=[anywhere] * len(kept),
        out_specs=[near] * len(kept),
        scratch_shapes=[pltpu.SemaphoreType.DMA((len(kept),))],
        compiler_params=pltpu.CompilerParams(vmem_limit_bytes=STAGE),
        cost_estimate=pl.CostEstimate(
            flops=2**30, bytes_accessed=2**24, transcendentals=0
        ),
        interpret=INTERPRET,
        name="stage",
    )(*kept)
    sent = pl.pallas_call(
        functools.partial(middle_kernel, unitary),
        out_shape=jax.ShapeDtypeStruct((groups_x, groups_z, step + groups, LANES), bf16),
        in_specs=[near] * 3,
        out_specs=near,
        scratch_shapes=[
            pltpu.VMEM((devices * groups, LANES), f32),
            pltpu.VMEM(((2 * rows + 1) * PADDED, owned * devices), bf16),
            pltpu.VMEM((owned * devices, side), bf16),
            pltpu.VMEM(((2 * rows + 1) * PADDED, side), bf16),
            pltpu.VMEM((2, groups_x, rows, groups, side), f32),
            pltpu.VMEM((2, groups_x, rows, groups, LANES), f32),
            pltpu.VMEM((2 * half_rows, side), bf16),
            pltpu.VMEM((2 * half_rows, width), bf16),
            pltpu.VMEM((2, groups_x, rows, groups, LANES), f32),
            pltpu.VMEM((half_rows, width), f32),
            pltpu.VMEM((2, groups_x, rows, groups, side), f32),
            pltpu.VMEM((rows, LANES, devices), f32),
        ],
        compiler_params=pltpu.CompilerParams(vmem_limit_bytes=MIDDLE),
        interpret=INTERPRET,
        name="middle",
    )(
        got.reshape(groups_x, groups_z, 2 * step + groups, LANES),
        tables,
        staged_x,
    )
    got = lax.all_to_all(
        sent.reshape(devices, step + groups, LANES), AXES, 0, 0, tiled=True
    )

    high_term, low_response = pl.pallas_call(
        finish_kernel,
        out_shape=(
            jax.ShapeDtypeStruct((groups, LANES, levels), bf16),
            jax.ShapeDtypeStruct((owned, levels), f32),
        ),
        in_specs=[near] * 2,
        out_specs=(anywhere, near),
        scratch_shapes=[
            pltpu.VMEM((LANES * groups, LANES), f32),
            pltpu.VMEM((devices * groups, LANES), f32),
            pltpu.VMEM((levels, LANES), f32),
            pltpu.VMEM((groups, LANES, levels), bf16),
            pltpu.SemaphoreType.DMA((devices * rows // LANES,)),
        ],
        compiler_params=pltpu.CompilerParams(vmem_limit_bytes=FINISH),
        interpret=INTERPRET,
        name="finish",
    )(got, tau_inverse)
    return (high_term.reshape(cells_x, cells_z, levels), low_response)


def solution(mesh):
    placed = (
        P("gx", "gz", None),
        P("gx", "gz", None),
        P(AXES, None),
        P(AXES, None),
        P(AXES),
        P(AXES),
        P(AXES, None, None),
    )
    return jax.shard_map(
        on_device,
        mesh=mesh,
        in_specs=placed,
        out_specs=(P("gx", "gz", None), P(AXES, None)),
        check_vma=False,
    )
```

```python
import functools
import math

import jax
import jax.numpy as jnp
from jax import lax
from jax.experimental import pallas as pl
from jax.experimental.pallas import tpu as pltpu
from jax.sharding import PartitionSpec as P

KL = 32
SIDE = 2 * KL + 1
PADDED = 80
LANES = 128
HALF = LANES // 2
AXES = ("gx", "gz")
INTERPRET = False
MIB = 1024 * 1024
WHOLE = 67043328
PREPARE = WHOLE
MIDDLE = 24 * MIB
STAGE = 16 * MIB
FINISH = 16 * MIB
bf16 = jnp.bfloat16
f32 = jnp.float32


def axis_table(index, positions, length):
    wavenum = jnp.where(index <= KL, index, index - KL)
    phases = wavenum[:, None] * positions[None, :] % length
    angles = phases.astype(f32) * (2.0 * math.pi / length)
    return jnp.where((index <= KL)[:, None], jnp.cos(angles), jnp.sin(angles))


def split(values):
    top = lax.reduce_precision(values, 8, 7)
    return top.astype(bf16), (values - top).astype(bf16)


def halves(values):
    top = values.astype(bf16)
    return top, (values - top.astype(f32)).astype(bf16)


def dot(a, b):
    return jnp.dot(a, b, preferred_element_type=f32)


def x_tables(groups_x, groups, group, length_x):
    part = jnp.arange(group, dtype=jnp.int32)[:, None, None]
    device = jnp.arange(groups_x, dtype=jnp.int32)[None, :, None]
    block = jnp.arange(groups, dtype=jnp.int32)[None, None, :]
    where_x = (device * (group * groups) + block * group + part).reshape(-1)
    index = jnp.arange(PADDED, dtype=jnp.int32)
    table = axis_table(index, where_x, length_x)
    table = jnp.where((index < SIDE)[:, None], table, 0.0)
    top, rest = split(table)
    forward = jnp.concatenate([top, rest], axis=0)
    top, rest = split(table.T)
    return forward, jnp.concatenate([top, rest], axis=1)


def z_table(group, cells_z, length_z):
    column = jnp.arange(length_z * group, dtype=jnp.int32)
    where_z = column // (group * cells_z) * cells_z + column % cells_z
    index = 1 + jnp.arange(LANES, dtype=jnp.int32) % HALF
    return axis_table(index, where_z, length_z).T.astype(bf16)


def across(eye, block):
    return lax.dot_general(
        eye, block, (((1,), (1,)), ((), ())), preferred_element_type=f32
    )


def identity(size):
    return (
        lax.broadcasted_iota(jnp.int32, (size, size), 0)
        == lax.broadcasted_iota(jnp.int32, (size, size), 1)
    ).astype(bf16)


def prepare_kernel(
    u_ref,
    v_ref,
    low_u_ref,
    low_v_ref,
    kx_ref,
    kz_ref,
    out_ref,
    fine,
    lows,
    index,
    tall,
    low,
    tile,
    ready,
    fine_sem,
    low_sem,
    index_sem,
    out_sem,
):
    groups, _, levels = u_ref.shape
    owned = low_u_ref.shape[0]
    devices = out_ref.shape[0]
    rows = levels // devices
    step = rows * groups
    side = 2 * LANES
    pairs = groups // 2
    copies = []
    for k, ref in enumerate((kx_ref, kz_ref)):
        copies.append(pltpu.make_async_copy(ref, index.at[k], index_sem.at[k]))
    for k, ref in enumerate((low_u_ref, low_v_ref)):
        copies.append(pltpu.make_async_copy(ref, lows.at[k], low_sem.at[k]))
    for k, ref in enumerate((u_ref, v_ref)):
        for g in range(pairs):
            at = pl.ds(2 * g, 2)
            copies.append(
                pltpu.make_async_copy(ref.at[at], fine.at[k, at], fine_sem.at[k, g])
            )
    for copy in copies[4 : 4 + pairs] + copies[:4]:
        copy.start()

    def send(k, first, count):
        part = (slice(None), pl.ds(first, count))
        return pltpu.make_async_copy(ready.at[part], out_ref.at[part], out_sem.at[k])

    sends = []
    for k in range(2):
        for g in range(pairs):
            copies[4 + k * pairs + g].wait()
            if k + g == 0:
                for copy in copies[4 + pairs :]:
                    copy.start()
            block = fine[k, 2 * g : 2 * g + 2].reshape(side, levels)
            for y in range(0, levels, side):
                turned = block[:, y : y + side].astype(f32).T
                at = y * groups + 2 * g
                tall[pl.ds(at, side, stride=groups), :] = turned[:, :LANES]
                tall[pl.ds(at + 1, side, stride=groups), :] = turned[:, LANES:]
        ready[:, k * step : (k + 1) * step, :] = (
            tall[...].astype(bf16).reshape(devices, step, LANES)
        )
        sends.append(send(k, k * step, step))
        sends[-1].start()
        if k == 1:
            continue
        for copy in copies[:4]:
            copy.wait()
        lane = lax.broadcasted_iota(jnp.int32, (1, LANES), 1)
        line = jnp.zeros((1, LANES), f32)
        for m in range(owned):
            line = jnp.where(lane == owned + m, index[0, m].astype(f32), line)
            line = jnp.where(lane == 2 * owned + m, index[1, m].astype(f32), line)
        small = identity(LANES)
        for h in range(2):
            padded = jnp.concatenate(
                [lows[h].astype(f32), jnp.zeros((LANES - owned, levels), f32)], axis=0
            ).astype(bf16)
            for y in range(0, levels, LANES):
                low[pl.ds(y, LANES), :] = across(small, padded[:, y : y + LANES])
            for y in range(rows):
                tile[pl.ds(h * rows + y, devices, stride=groups), :] = (
                    low[pl.ds(y, devices, stride=rows), :] + line
                )
        ready[:, 2 * step :, :] = tile[...].astype(bf16).reshape(devices, groups, LANES)
        sends.append(send(2, 2 * step, groups))
        sends[-1].start()
    for copy in sends:
        copy.wait()


def middle_kernel(
    unitary,
    got_ref,
    x_ref,
    back_x_ref,
    base_ref,
    out_ref,
    table,
    modes,
    left,
    right,
    spectrum,
    wave,
    mean,
    wave_top,
    products,
    sums,
    cross,
    coefficients,
    picked,
):
    groups_x, groups_z, _, _ = got_ref.shape
    groups = 8
    rows = 4
    owned = 16
    devices = groups_x * groups_z
    step = rows * groups
    points = groups_x * groups
    side = 2 * LANES
    half_rows = groups_x * step
    lane = lax.broadcasted_iota(jnp.int32, (1, LANES), 1)
    low_half = lane < HALF
    which = lane // (LANES // 4)

    width = groups_z * LANES
    owner = lax.broadcasted_iota(jnp.int32, (LANES, side), 0) // (LANES // 4)
    part = lax.broadcasted_iota(jnp.int32, (LANES, side), 1) // HALF
    own = jnp.where(owner == part, 1.0, 0.0).astype(bf16)
    for j in range(groups_z):
        at = slice(j * LANES, (j + 1) * LANES)
        table[at, :] = jnp.concatenate([base_ref[at, :]] * 2, axis=1) * own

    modes[...] = got_ref[:, :, 2 * step :, :].astype(f32).reshape(devices * groups, LANES)
    first = modes[pl.ds(0, devices, stride=groups), :]
    turned = [first.T]
    for c in range(1, 2 * rows):
        turned.append(modes[pl.ds(c, devices, stride=groups), :].T)
    row = lax.broadcasted_iota(jnp.int32, (PADDED, devices), 0).astype(f32)
    column = lax.broadcasted_iota(jnp.int32, (devices, LANES), 1)
    wanted = (1 + column % HALF).astype(f32)
    for m in range(owned):
        at = slice(m * devices, (m + 1) * devices)
        hit = row == turned[0][owned + m : owned + m + 1, :]
        hit = jnp.where(hit, 1.0, 0.0).astype(bf16)
        for c in range(2 * rows):
            value = jnp.broadcast_to(turned[c][m : m + 1, :], (16, devices)).astype(bf16)
            value = jnp.concatenate([value] * (PADDED // 16), axis=0)
            left[c * PADDED : (c + 1) * PADDED, at] = hit * value
        left[2 * rows * PADDED :, at] = hit
        index_z = jnp.broadcast_to(
            first[:, 2 * owned + m : 2 * owned + m + 1], (devices, LANES)
        )
        right[at, :LANES] = jnp.where(wanted == index_z, 1.0, 0.0).astype(bf16)
        right[at, LANES:] = jnp.where(index_z == 0.0, 1.0, 0.0).astype(bf16)
    spectrum[...] = dot(left[...], right[...]).astype(bf16)

    def spread(k, parts):
        both = jnp.concatenate(parts, axis=1)
        full = dot(back_x_ref[...], jnp.concatenate([both, both], axis=0))
        for y in range(len(parts)):
            part = [
                full[p * points : (p + 1) * points, y * side : (y + 1) * side]
                for p in range(4)
            ]
            waves = jnp.concatenate(
                [
                    jnp.where(low_half, part[0][:, :LANES], part[1][:, :LANES]),
                    jnp.where(low_half, part[2][:, :LANES], part[3][:, :LANES]),
                ],
                axis=1,
            )
            constant = part[3][:, LANES:]
            for p in range(3):
                constant = jnp.where(which == p, part[p][:, LANES:], constant)
            wave[k, :, y] = waves.reshape(groups_x, groups, side)
            mean[k, :, y] = constant.reshape(groups_x, groups, LANES)

    for k in range(2):
        spread(
            k,
            [
                spectrum[(k * rows + y) * PADDED : (k * rows + y + 1) * PADDED, :]
                for y in range(rows)
            ],
        )
    wave_top[...] = wave[...].reshape(2 * half_rows, side).astype(bf16)
    sums[...] = jnp.zeros_like(sums)

    def fine(j, k):
        parts = [
            got_ref[:, 2 * j + e, k * step : (k + 1) * step, :].reshape(half_rows, LANES)
            for e in range(2)
        ]
        return jnp.concatenate(parts, axis=1).astype(f32)

    def multiply(j, _):
        at = pl.ds(pl.multiple_of(j * side, side), side)
        coarse = across(wave_top[...], table[at, :])
        flat = mean[...].reshape(2 * half_rows, LANES)
        coarse = coarse + jnp.concatenate([flat, flat], axis=1)
        coarse_u, coarse_v = coarse[:half_rows], coarse[half_rows:]
        fine_u, fine_v = fine(j, 0), fine(j, 1)
        self_term = (coarse_u * coarse_v + fine_u * fine_v).astype(bf16)
        cross_term = coarse_u * fine_v + fine_u * coarse_v
        cross[:, at] = cross_term
        cross_round = cross_term.astype(bf16)
        products[:half_rows, at] = self_term
        products[half_rows:, at] = cross_round
        for k, term in enumerate((self_term, cross_round)):
            wide = term.astype(f32)
            sums[k] += (wide[:, :LANES] + wide[:, LANES:]).reshape(
                groups_x, rows, groups, LANES
            )
        return 0

    lax.fori_loop(0, groups_z // 2, multiply, 0, unroll=1)
    both = dot(products[...], table[...])
    coefficients[...] = both.reshape(2, groups_x, rows, groups, side)

    def project(k):
        stacks = []
        for y in range(rows):
            waves = coefficients[k, :, y].reshape(points, side)
            total = sums[k, :, y].reshape(points, LANES)
            stack = []
            for part in range(4):
                half = waves[:, :LANES] if part < 2 else waves[:, LANES:]
                keep = low_half if part % 2 == 0 else jnp.logical_not(low_half)
                stack.append(
                    jnp.concatenate(
                        [
                            jnp.where(keep, half, 0.0),
                            jnp.where(which == part, total, 0.0),
                        ],
                        axis=1,
                    )
                )
            stacks.append(jnp.concatenate(stack, axis=0))
        top, rest = halves(jnp.concatenate(stacks, axis=1))
        table_x = x_ref[...]
        outer = dot(table_x, top)
        outer = outer[:PADDED] + outer[PADDED:] + dot(table_x[:PADDED], rest)
        done = []
        for y in range(rows):
            waves = outer[:, y * side : y * side + LANES] * unitary
            waves = waves + pltpu.roll(waves, HALF, 1)
            constant = outer[:, y * side + LANES : (y + 1) * side]
            constant = jnp.sum(constant, axis=1, keepdims=True) * unitary
            done.append((waves, jnp.broadcast_to(constant, (PADDED, LANES))))
        return done

    row_index = lax.broadcasted_iota(jnp.int32, (PADDED, 1), 0)
    weight_x = jnp.where(row_index > 0, 2.0, 1.0).astype(f32)
    mask = spectrum[2 * rows * PADDED :, :]
    parts = []
    for waves, constant in project(1):
        low = jnp.concatenate([waves * (2.0 * weight_x), constant * weight_x], axis=1)
        parts.append(low.astype(bf16) * mask)
    spread(0, parts)
    wave_top[:half_rows] = wave[0].reshape(half_rows, side).astype(bf16)

    def subtract(j, _):
        at = pl.ds(pl.multiple_of(j * side, side), side)
        restored = across(wave_top[:half_rows], table[at, :])
        flat = mean[0].reshape(half_rows, LANES)
        restored = restored + jnp.concatenate([flat, flat], axis=1)
        high = (cross[:, at] - unitary * restored).astype(bf16)
        for e in range(2):
            out_ref[:, 2 * j + e, :step, :] = high[:, e * LANES : (e + 1) * LANES].reshape(
                groups_x, step, LANES
            )
        return 0

    lax.fori_loop(0, groups_z // 2, subtract, 0, unroll=1)

    lines = 72
    parts = []
    for waves, constant in project(0):
        force = jnp.where(low_half, waves, jnp.where(lane == HALF, constant, 0.0))
        force = jnp.concatenate([force, jnp.zeros((LANES - PADDED, LANES), f32)], axis=0)
        parts.append(force.T[:lines])
    force = jnp.concatenate(parts, axis=0).astype(bf16)[:, :PADDED]
    line = lax.broadcasted_iota(jnp.int32, (lines, devices), 0)
    line = jnp.where(line < HALF, line + 1, jnp.where(line == HALF, 0, -1)).astype(f32)
    picked[...] = jnp.zeros_like(picked)
    for m in range(0, owned, 2):
        chosen = dot(force, left[2 * rows * PADDED :, m * devices : (m + 2) * devices])
        for e in range(2):
            hit = line == turned[0][2 * owned + m + e : 2 * owned + m + e + 1, :]
            for y in range(rows):
                value = chosen[y * lines : (y + 1) * lines, e * devices : (e + 1) * devices]
                picked[y, m + e : m + e + 1, :] = jnp.sum(
                    jnp.where(hit, value, 0.0), axis=0, keepdims=True
                )
    modes[...] = jnp.zeros_like(modes)
    for y in range(rows):
        modes[pl.ds(y, devices, stride=groups), :] = picked[y].T
    out_ref[:, :, step:, :] = (
        modes[...].astype(bf16).reshape(groups_x, groups_z, groups, LANES)
    )


def finish_kernel(got_ref, tau_ref, high_hbm, low_ref, tall, tile, force, ready, out_sem):
    devices = got_ref.shape[0]
    owned, levels, _ = tau_ref.shape
    rows = levels // devices
    groups = high_hbm.shape[0]
    step = rows * groups
    chunk = LANES // rows
    sends = []
    for q in range(devices // chunk):
        at = slice(q * chunk, (q + 1) * chunk)
        tall[...] = got_ref[at, :step, :].astype(f32).reshape(chunk * step, LANES)
        where = slice(q * LANES, (q + 1) * LANES)
        for g in range(groups):
            column = tall[pl.ds(g, LANES, stride=groups), :]
            ready[g, :, where] = column.T.astype(bf16)
        part = (slice(None), slice(None), pl.ds(q * LANES, LANES))
        sends.append(
            pltpu.make_async_copy(ready.at[part], high_hbm.at[part], out_sem.at[q])
        )
        sends[-1].start()
    tile[...] = got_ref[:, step:, :].astype(f32).reshape(devices * groups, LANES)
    for y in range(rows):
        force[pl.ds(y, devices, stride=rows), :] = tile[
            pl.ds(y, devices, stride=groups), :
        ]
    vector = force[...].astype(bf16)
    lane = lax.broadcasted_iota(jnp.int32, (1, LANES), 1)
    answer = jnp.zeros((levels, LANES), f32)
    for m in range(0, owned, 2):
        pair = dot(tau_ref[m : m + 2].reshape(2 * levels, levels), vector)
        answer = jnp.where(lane == m, pair[:levels], answer)
        answer = jnp.where(lane == m + 1, pair[levels:], answer)
    low_ref[...] = answer.T[:owned]
    for copy in sends:
        copy.wait()


def stage_kernel(*refs):
    count = (len(refs) - 1) // 2
    copies = [
        pltpu.make_async_copy(refs[k], refs[count + k], refs[-1].at[k])
        for k in range(count)
    ]
    for copy in copies:
        copy.start()
    for copy in copies:
        copy.wait()


def on_device(high_u, high_v, low_u, low_v, low_kx, low_kz, tau_inverse):
    cells_x, cells_z, levels = high_u.shape
    owned = low_u.shape[0]
    groups_x = lax.axis_size("gx")
    groups_z = lax.axis_size("gz")
    devices = groups_x * groups_z
    length_x = groups_x * cells_x
    length_z = groups_z * cells_z
    rows = levels // devices
    group = LANES // cells_z
    groups = cells_x // group
    step = rows * groups
    points = groups_x * groups
    half_rows = groups_x * step
    width = groups_z * LANES
    side = 2 * LANES
    unitary = 1.0 / math.sqrt(length_x * length_z)

    anywhere = pl.BlockSpec(memory_space=pltpu.HBM)
    near = pl.BlockSpec(memory_space=pltpu.VMEM)
    sent = pl.pallas_call(
        prepare_kernel,
        out_shape=jax.ShapeDtypeStruct((devices, 2 * step + groups, LANES), bf16),
        in_specs=[anywhere] * 6,
        out_specs=anywhere,
        scratch_shapes=[
            pltpu.VMEM((2, groups, LANES, levels), bf16),
            pltpu.VMEM((2, owned, levels), bf16),
            pltpu.SMEM((2, owned), jnp.int32),
            pltpu.VMEM((levels * groups, LANES), f32),
            pltpu.VMEM((levels, LANES), f32),
            pltpu.VMEM((devices * groups, LANES), f32),
            pltpu.VMEM((devices, 2 * step + groups, LANES), bf16),
            pltpu.SemaphoreType.DMA((2, groups // 2)),
            pltpu.SemaphoreType.DMA((2,)),
            pltpu.SemaphoreType.DMA((2,)),
            pltpu.SemaphoreType.DMA((3,)),
        ],
        compiler_params=pltpu.CompilerParams(vmem_limit_bytes=PREPARE),
        interpret=INTERPRET,
        name="prepare",
    )(
        high_u.reshape(groups, LANES, levels),
        high_v.reshape(groups, LANES, levels),
        low_u,
        low_v,
        low_kx,
        low_kz,
    )
    got = lax.all_to_all(sent, AXES, 0, 0, tiled=True)

    forward_x, back_x = x_tables(groups_x, groups, group, length_x)
    kept = (forward_x, back_x, z_table(group, cells_z, length_z))
    tables = pl.pallas_call(
        stage_kernel,
        out_shape=[jax.ShapeDtypeStruct(a.shape, a.dtype) for a in kept],
        in_specs=[anywhere] * len(kept),
        out_specs=[near] * len(kept),
        scratch_shapes=[pltpu.SemaphoreType.DMA((len(kept),))],
        compiler_params=pltpu.CompilerParams(vmem_limit_bytes=STAGE),
        cost_estimate=pl.CostEstimate(
            flops=2**30, bytes_accessed=2**24, transcendentals=0
        ),
        interpret=INTERPRET,
        name="stage",
    )(*kept)
    sent = pl.pallas_call(
        functools.partial(middle_kernel, unitary),
        out_shape=jax.ShapeDtypeStruct((groups_x, groups_z, step + groups, LANES), bf16),
        in_specs=[near] * 4,
        out_specs=near,
        scratch_shapes=[
            pltpu.VMEM((width, side), bf16),
            pltpu.VMEM((devices * groups, LANES), f32),
            pltpu.VMEM(((2 * rows + 1) * PADDED, owned * devices), bf16),
            pltpu.VMEM((owned * devices, side), bf16),
            pltpu.VMEM(((2 * rows + 1) * PADDED, side), bf16),
            pltpu.VMEM((2, groups_x, rows, groups, side), f32),
            pltpu.VMEM((2, groups_x, rows, groups, LANES), f32),
            pltpu.VMEM((2 * half_rows, side), bf16),
            pltpu.VMEM((2 * half_rows, width), bf16),
            pltpu.VMEM((2, groups_x, rows, groups, LANES), f32),
            pltpu.VMEM((half_rows, width), f32),
            pltpu.VMEM((2, groups_x, rows, groups, side), f32),
            pltpu.VMEM((rows, LANES, devices), f32),
        ],
        compiler_params=pltpu.CompilerParams(vmem_limit_bytes=MIDDLE),
        cost_estimate=pl.CostEstimate(
            flops=2**33, bytes_accessed=2**22, transcendentals=0
        ),
        interpret=INTERPRET,
        name="middle",
    )(
        got.reshape(groups_x, groups_z, 2 * step + groups, LANES),
        *tables,
    )
    got = lax.all_to_all(
        sent.reshape(devices, step + groups, LANES), AXES, 0, 0, tiled=True
    )

    high_term, low_response = pl.pallas_call(
        finish_kernel,
        out_shape=(
            jax.ShapeDtypeStruct((groups, LANES, levels), bf16),
            jax.ShapeDtypeStruct((owned, levels), f32),
        ),
        in_specs=[near] * 2,
        out_specs=(anywhere, near),
        scratch_shapes=[
            pltpu.VMEM((LANES * groups, LANES), f32),
            pltpu.VMEM((devices * groups, LANES), f32),
            pltpu.VMEM((levels, LANES), f32),
            pltpu.VMEM((groups, LANES, levels), bf16),
            pltpu.SemaphoreType.DMA((devices * rows // LANES,)),
        ],
        compiler_params=pltpu.CompilerParams(vmem_limit_bytes=FINISH),
        interpret=INTERPRET,
        name="finish",
    )(got, tau_inverse)
    return (high_term.reshape(cells_x, cells_z, levels), low_response)


def solution(mesh):
    placed = (
        P("gx", "gz", None),
        P("gx", "gz", None),
        P(AXES, None),
        P(AXES, None),
        P(AXES),
        P(AXES),
        P(AXES, None, None),
    )
    return jax.shard_map(
        on_device,
        mesh=mesh,
        in_specs=placed,
        out_specs=(P("gx", "gz", None), P(AXES, None)),
        check_vma=False,
    )
```

```python
import functools
import math

import jax
import jax.numpy as jnp
from jax import lax
from jax.experimental import pallas as pl
from jax.experimental.pallas import tpu as pltpu
from jax.sharding import PartitionSpec as P

KL = 32
SIDE = 2 * KL + 1
PADDED = 80
LANES = 128
HALF = LANES // 2
AXES = ("gx", "gz")
INTERPRET = False
MIB = 1024 * 1024
WHOLE = 67043328
PREPARE = WHOLE
MIDDLE = 24 * MIB
STAGE = 16 * MIB
FINISH = 16 * MIB
bf16 = jnp.bfloat16
f32 = jnp.float32


def axis_table(index, positions, length):
    wavenum = jnp.where(index <= KL, index, index - KL)
    phases = wavenum[:, None] * positions[None, :] % length
    angles = phases.astype(f32) * (2.0 * math.pi / length)
    return jnp.where((index <= KL)[:, None], jnp.cos(angles), jnp.sin(angles))


def split(values):
    top = lax.reduce_precision(values, 8, 7)
    return top.astype(bf16), (values - top).astype(bf16)


def halves(values):
    top = values.astype(bf16)
    return top, (values - top.astype(f32)).astype(bf16)


def dot(a, b):
    return jnp.dot(a, b, preferred_element_type=f32)


def x_tables(groups_x, groups, group, length_x):
    part = jnp.arange(group, dtype=jnp.int32)[:, None, None]
    device = jnp.arange(groups_x, dtype=jnp.int32)[None, :, None]
    block = jnp.arange(groups, dtype=jnp.int32)[None, None, :]
    where_x = (device * (group * groups) + block * group + part).reshape(-1)
    index = jnp.arange(PADDED, dtype=jnp.int32)
    table = axis_table(index, where_x, length_x)
    table = jnp.where((index < SIDE)[:, None], table, 0.0)
    top, rest = split(table)
    forward = jnp.concatenate([top, rest], axis=0)
    top, rest = split(table.T)
    return forward, jnp.concatenate([top, rest], axis=1)


def z_table(group, cells_z, length_z):
    column = jnp.arange(length_z * group, dtype=jnp.int32)
    where_z = column // (group * cells_z) * cells_z + column % cells_z
    index = 1 + jnp.arange(LANES, dtype=jnp.int32) % HALF
    return axis_table(index, where_z, length_z).T.astype(bf16)


def across(eye, block):
    return lax.dot_general(
        eye, block, (((1,), (1,)), ((), ())), preferred_element_type=f32
    )


def identity(size):
    return (
        lax.broadcasted_iota(jnp.int32, (size, size), 0)
        == lax.broadcasted_iota(jnp.int32, (size, size), 1)
    ).astype(bf16)


def prepare_kernel(
    u_ref,
    v_ref,
    low_u_ref,
    low_v_ref,
    kx_ref,
    kz_ref,
    out_ref,
    fine,
    lows,
    index,
    tall,
    low,
    tile,
    ready,
    fine_sem,
    low_sem,
    index_sem,
    out_sem,
):
    groups, _, levels = u_ref.shape
    owned = low_u_ref.shape[0]
    devices = out_ref.shape[0]
    rows = levels // devices
    step = rows * groups
    side = 2 * LANES
    pairs = groups // 2
    copies = []
    for k, ref in enumerate((kx_ref, kz_ref)):
        copies.append(pltpu.make_async_copy(ref, index.at[k], index_sem.at[k]))
    for k, ref in enumerate((low_u_ref, low_v_ref)):
        copies.append(pltpu.make_async_copy(ref, lows.at[k], low_sem.at[k]))
    for k, ref in enumerate((u_ref, v_ref)):
        for g in range(pairs):
            at = pl.ds(2 * g, 2)
            copies.append(
                pltpu.make_async_copy(ref.at[at], fine.at[k, at], fine_sem.at[k, g])
            )
    for copy in copies[4 : 4 + pairs] + copies[:4]:
        copy.start()

    def send(k, first, count):
        part = (slice(None), pl.ds(first, count))
        return pltpu.make_async_copy(ready.at[part], out_ref.at[part], out_sem.at[k])

    sends = []
    for k in range(2):
        for g in range(pairs):
            copies[4 + k * pairs + g].wait()
            if k + g == 0:
                for copy in copies[4 + pairs :]:
                    copy.start()
            block = fine[k, 2 * g : 2 * g + 2].reshape(side, levels)
            for y in range(0, levels, side):
                turned = block[:, y : y + side].astype(f32).T
                at = y * groups + 2 * g
                tall[pl.ds(at, side, stride=groups), :] = turned[:, :LANES]
                tall[pl.ds(at + 1, side, stride=groups), :] = turned[:, LANES:]
        ready[:, k * step : (k + 1) * step, :] = (
            tall[...].astype(bf16).reshape(devices, step, LANES)
        )
        sends.append(send(k, k * step, step))
        sends[-1].start()
        if k == 1:
            continue
        for copy in copies[:4]:
            copy.wait()
        lane = lax.broadcasted_iota(jnp.int32, (1, LANES), 1)
        line = jnp.zeros((1, LANES), f32)
        for m in range(owned):
            line = jnp.where(lane == owned + m, index[0, m].astype(f32), line)
            line = jnp.where(lane == 2 * owned + m, index[1, m].astype(f32), line)
        small = identity(LANES)
        for h in range(2):
            padded = jnp.concatenate(
                [lows[h].astype(f32), jnp.zeros((LANES - owned, levels), f32)], axis=0
            ).astype(bf16)
            for y in range(0, levels, LANES):
                low[pl.ds(y, LANES), :] = across(small, padded[:, y : y + LANES])
            for y in range(rows):
                tile[pl.ds(h * rows + y, devices, stride=groups), :] = (
                    low[pl.ds(y, devices, stride=rows), :] + line
                )
        ready[:, 2 * step :, :] = tile[...].astype(bf16).reshape(devices, groups, LANES)
        sends.append(send(2, 2 * step, groups))
        sends[-1].start()
    for copy in sends:
        copy.wait()


def middle_kernel(
    unitary,
    got_ref,
    x_ref,
    back_x_ref,
    base_ref,
    out_ref,
    table,
    modes,
    left,
    right,
    spectrum,
    wave,
    mean,
    wave_top,
    products,
    sums,
    cross,
    coefficients,
    picked,
):
    groups_x, groups_z, _, _ = got_ref.shape
    groups = 8
    rows = 4
    owned = 16
    devices = groups_x * groups_z
    step = rows * groups
    points = groups_x * groups
    side = 2 * LANES
    half_rows = groups_x * step
    lane = lax.broadcasted_iota(jnp.int32, (1, LANES), 1)
    low_half = lane < HALF
    which = lane // (LANES // 4)

    width = groups_z * LANES
    owner = lax.broadcasted_iota(jnp.int32, (LANES, side), 0) // (LANES // 4)
    part = lax.broadcasted_iota(jnp.int32, (LANES, side), 1) // HALF
    own = jnp.where(owner == part, 1.0, 0.0).astype(bf16)
    for j in range(groups_z):
        at = slice(j * LANES, (j + 1) * LANES)
        table[at, :] = jnp.concatenate([base_ref[at, :]] * 2, axis=1) * own

    modes[...] = got_ref[:, :, 2 * step :, :].astype(f32).reshape(devices * groups, LANES)
    first = modes[pl.ds(0, devices, stride=groups), :]
    turned = [first.T]
    for c in range(1, 2 * rows):
        turned.append(modes[pl.ds(c, devices, stride=groups), :].T)
    row = lax.broadcasted_iota(jnp.int32, (PADDED, devices), 0).astype(f32)
    column = lax.broadcasted_iota(jnp.int32, (devices, LANES), 1)
    wanted = (1 + column % HALF).astype(f32)
    for m in range(owned):
        at = slice(m * devices, (m + 1) * devices)
        hit = row == turned[0][owned + m : owned + m + 1, :]
        hit = jnp.where(hit, 1.0, 0.0).astype(bf16)
        for c in range(2 * rows):
            value = jnp.broadcast_to(turned[c][m : m + 1, :], (16, devices)).astype(bf16)
            value = jnp.concatenate([value] * (PADDED // 16), axis=0)
            left[c * PADDED : (c + 1) * PADDED, at] = hit * value
        left[2 * rows * PADDED :, at] = hit
        index_z = jnp.broadcast_to(
            first[:, 2 * owned + m : 2 * owned + m + 1], (devices, LANES)
        )
        right[at, :LANES] = jnp.where(wanted == index_z, 1.0, 0.0).astype(bf16)
        right[at, LANES:] = jnp.where(index_z == 0.0, 1.0, 0.0).astype(bf16)
    spectrum[...] = dot(left[...], right[...]).astype(bf16)

    def spread(k, parts):
        both = jnp.concatenate(parts, axis=1)
        full = dot(back_x_ref[...], jnp.concatenate([both, both], axis=0))
        for y in range(len(parts)):
            part = [
                full[p * points : (p + 1) * points, y * side : (y + 1) * side]
                for p in range(4)
            ]
            waves = jnp.concatenate(
                [
                    jnp.where(low_half, part[0][:, :LANES], part[1][:, :LANES]),
                    jnp.where(low_half, part[2][:, :LANES], part[3][:, :LANES]),
                ],
                axis=1,
            )
            constant = part[3][:, LANES:]
            for p in range(3):
                constant = jnp.where(which == p, part[p][:, LANES:], constant)
            wave[k, :, y] = waves.reshape(groups_x, groups, side)
            mean[k, :, y] = constant.reshape(groups_x, groups, LANES)

    for k in range(2):
        spread(
            k,
            [
                spectrum[(k * rows + y) * PADDED : (k * rows + y + 1) * PADDED, :]
                for y in range(rows)
            ],
        )
    wave_top[...] = wave[...].reshape(2 * half_rows, side).astype(bf16)
    sums[...] = jnp.zeros_like(sums)

    def fine(j, k):
        parts = [
            got_ref[:, 2 * j + e, k * step : (k + 1) * step, :].reshape(half_rows, LANES)
            for e in range(2)
        ]
        return jnp.concatenate(parts, axis=1).astype(f32)

    def multiply(j, _):
        at = pl.ds(pl.multiple_of(j * side, side), side)
        coarse = across(wave_top[...], table[at, :])
        flat = mean[...].reshape(2 * half_rows, LANES)
        coarse = coarse + jnp.concatenate([flat, flat], axis=1)
        coarse_u, coarse_v = coarse[:half_rows], coarse[half_rows:]
        fine_u, fine_v = fine(j, 0), fine(j, 1)
        self_term = (coarse_u * coarse_v + fine_u * fine_v).astype(bf16)
        cross_term = coarse_u * fine_v + fine_u * coarse_v
        cross[:, at] = cross_term
        cross_round = cross_term.astype(bf16)
        products[:half_rows, at] = self_term
        products[half_rows:, at] = cross_round
        for k, term in enumerate((self_term, cross_round)):
            wide = term.astype(f32)
            sums[k] += (wide[:, :LANES] + wide[:, LANES:]).reshape(
                groups_x, rows, groups, LANES
            )
        return 0

    lax.fori_loop(0, groups_z // 2, multiply, 0, unroll=8)
    both = dot(products[...], table[...])
    coefficients[...] = both.reshape(2, groups_x, rows, groups, side)

    def project(k):
        stacks = []
        for y in range(rows):
            waves = coefficients[k, :, y].reshape(points, side)
            total = sums[k, :, y].reshape(points, LANES)
            stack = []
            for part in range(4):
                half = waves[:, :LANES] if part < 2 else waves[:, LANES:]
                keep = low_half if part % 2 == 0 else jnp.logical_not(low_half)
                stack.append(
                    jnp.concatenate(
                        [
                            jnp.where(keep, half, 0.0),
                            jnp.where(which == part, total, 0.0),
                        ],
                        axis=1,
                    )
                )
            stacks.append(jnp.concatenate(stack, axis=0))
        top, rest = halves(jnp.concatenate(stacks, axis=1))
        table_x = x_ref[...]
        outer = dot(table_x, top)
        outer = outer[:PADDED] + outer[PADDED:] + dot(table_x[:PADDED], rest)
        done = []
        for y in range(rows):
            waves = outer[:, y * side : y * side + LANES] * unitary
            waves = waves + pltpu.roll(waves, HALF, 1)
            constant = outer[:, y * side + LANES : (y + 1) * side]
            constant = jnp.sum(constant, axis=1, keepdims=True) * unitary
            done.append((waves, jnp.broadcast_to(constant, (PADDED, LANES))))
        return done

    row_index = lax.broadcasted_iota(jnp.int32, (PADDED, 1), 0)
    weight_x = jnp.where(row_index > 0, 2.0, 1.0).astype(f32)
    mask = spectrum[2 * rows * PADDED :, :]
    parts = []
    for waves, constant in project(1):
        low = jnp.concatenate([waves * (2.0 * weight_x), constant * weight_x], axis=1)
        parts.append(low.astype(bf16) * mask)
    spread(0, parts)
    wave_top[:half_rows] = wave[0].reshape(half_rows, side).astype(bf16)

    def subtract(j, _):
        at = pl.ds(pl.multiple_of(j * side, side), side)
        restored = across(wave_top[:half_rows], table[at, :])
        flat = mean[0].reshape(half_rows, LANES)
        restored = restored + jnp.concatenate([flat, flat], axis=1)
        high = (cross[:, at] - unitary * restored).astype(bf16)
        for e in range(2):
            out_ref[:, 2 * j + e, :step, :] = high[:, e * LANES : (e + 1) * LANES].reshape(
                groups_x, step, LANES
            )
        return 0

    lax.fori_loop(0, groups_z // 2, subtract, 0, unroll=8)

    lines = 72
    parts = []
    for waves, constant in project(0):
        force = jnp.where(low_half, waves, jnp.where(lane == HALF, constant, 0.0))
        force = jnp.concatenate([force, jnp.zeros((LANES - PADDED, LANES), f32)], axis=0)
        parts.append(force.T[:lines])
    force = jnp.concatenate(parts, axis=0).astype(bf16)[:, :PADDED]
    line = lax.broadcasted_iota(jnp.int32, (lines, devices), 0)
    line = jnp.where(line < HALF, line + 1, jnp.where(line == HALF, 0, -1)).astype(f32)
    picked[...] = jnp.zeros_like(picked)
    for m in range(0, owned, 2):
        chosen = dot(force, left[2 * rows * PADDED :, m * devices : (m + 2) * devices])
        for e in range(2):
            hit = line == turned[0][2 * owned + m + e : 2 * owned + m + e + 1, :]
            for y in range(rows):
                value = chosen[y * lines : (y + 1) * lines, e * devices : (e + 1) * devices]
                picked[y, m + e : m + e + 1, :] = jnp.sum(
                    jnp.where(hit, value, 0.0), axis=0, keepdims=True
                )
    modes[...] = jnp.zeros_like(modes)
    for y in range(rows):
        modes[pl.ds(y, devices, stride=groups), :] = picked[y].T
    out_ref[:, :, step:, :] = (
        modes[...].astype(bf16).reshape(groups_x, groups_z, groups, LANES)
    )


def finish_kernel(got_ref, tau_ref, high_hbm, low_ref, tall, tile, force, ready, out_sem):
    devices = got_ref.shape[0]
    owned, levels, _ = tau_ref.shape
    rows = levels // devices
    groups = high_hbm.shape[0]
    step = rows * groups
    chunk = LANES // rows
    sends = []
    for q in range(devices // chunk):
        at = slice(q * chunk, (q + 1) * chunk)
        tall[...] = got_ref[at, :step, :].astype(f32).reshape(chunk * step, LANES)
        where = slice(q * LANES, (q + 1) * LANES)
        for g in range(groups):
            column = tall[pl.ds(g, LANES, stride=groups), :]
            ready[g, :, where] = column.T.astype(bf16)
        part = (slice(None), slice(None), pl.ds(q * LANES, LANES))
        sends.append(
            pltpu.make_async_copy(ready.at[part], high_hbm.at[part], out_sem.at[q])
        )
        sends[-1].start()
    tile[...] = got_ref[:, step:, :].astype(f32).reshape(devices * groups, LANES)
    for y in range(rows):
        force[pl.ds(y, devices, stride=rows), :] = tile[
            pl.ds(y, devices, stride=groups), :
        ]
    vector = force[...].astype(bf16)
    lane = lax.broadcasted_iota(jnp.int32, (1, LANES), 1)
    answer = jnp.zeros((levels, LANES), f32)
    for m in range(0, owned, 2):
        pair = dot(tau_ref[m : m + 2].reshape(2 * levels, levels), vector)
        answer = jnp.where(lane == m, pair[:levels], answer)
        answer = jnp.where(lane == m + 1, pair[levels:], answer)
    low_ref[...] = answer.T[:owned]
    for copy in sends:
        copy.wait()


def stage_kernel(*refs):
    count = (len(refs) - 1) // 2
    copies = [
        pltpu.make_async_copy(refs[k], refs[count + k], refs[-1].at[k])
        for k in range(count)
    ]
    for copy in copies:
        copy.start()
    for copy in copies:
        copy.wait()


def on_device(high_u, high_v, low_u, low_v, low_kx, low_kz, tau_inverse):
    cells_x, cells_z, levels = high_u.shape
    owned = low_u.shape[0]
    groups_x = lax.axis_size("gx")
    groups_z = lax.axis_size("gz")
    devices = groups_x * groups_z
    length_x = groups_x * cells_x
    length_z = groups_z * cells_z
    rows = levels // devices
    group = LANES // cells_z
    groups = cells_x // group
    step = rows * groups
    points = groups_x * groups
    half_rows = groups_x * step
    width = groups_z * LANES
    side = 2 * LANES
    unitary = 1.0 / math.sqrt(length_x * length_z)

    anywhere = pl.BlockSpec(memory_space=pltpu.HBM)
    near = pl.BlockSpec(memory_space=pltpu.VMEM)
    sent = pl.pallas_call(
        prepare_kernel,
        out_shape=jax.ShapeDtypeStruct((devices, 2 * step + groups, LANES), bf16),
        in_specs=[anywhere] * 6,
        out_specs=anywhere,
        scratch_shapes=[
            pltpu.VMEM((2, groups, LANES, levels), bf16),
            pltpu.VMEM((2, owned, levels), bf16),
            pltpu.SMEM((2, owned), jnp.int32),
            pltpu.VMEM((levels * groups, LANES), f32),
            pltpu.VMEM((levels, LANES), f32),
            pltpu.VMEM((devices * groups, LANES), f32),
            pltpu.VMEM((devices, 2 * step + groups, LANES), bf16),
            pltpu.SemaphoreType.DMA((2, groups // 2)),
            pltpu.SemaphoreType.DMA((2,)),
            pltpu.SemaphoreType.DMA((2,)),
            pltpu.SemaphoreType.DMA((3,)),
        ],
        compiler_params=pltpu.CompilerParams(vmem_limit_bytes=PREPARE),
        interpret=INTERPRET,
        name="prepare",
    )(
        high_u.reshape(groups, LANES, levels),
        high_v.reshape(groups, LANES, levels),
        low_u,
        low_v,
        low_kx,
        low_kz,
    )
    got = lax.all_to_all(sent, AXES, 0, 0, tiled=True)

    forward_x, back_x = x_tables(groups_x, groups, group, length_x)
    kept = (forward_x, back_x, z_table(group, cells_z, length_z))
    tables = pl.pallas_call(
        stage_kernel,
        out_shape=[jax.ShapeDtypeStruct(a.shape, a.dtype) for a in kept],
        in_specs=[anywhere] * len(kept),
        out_specs=[near] * len(kept),
        scratch_shapes=[pltpu.SemaphoreType.DMA((len(kept),))],
        compiler_params=pltpu.CompilerParams(vmem_limit_bytes=STAGE),
        cost_estimate=pl.CostEstimate(
            flops=2**30, bytes_accessed=2**24, transcendentals=0
        ),
        interpret=INTERPRET,
        name="stage",
    )(*kept)
    sent = pl.pallas_call(
        functools.partial(middle_kernel, unitary),
        out_shape=jax.ShapeDtypeStruct((groups_x, groups_z, step + groups, LANES), bf16),
        in_specs=[near] * 4,
        out_specs=near,
        scratch_shapes=[
            pltpu.VMEM((width, side), bf16),
            pltpu.VMEM((devices * groups, LANES), f32),
            pltpu.VMEM(((2 * rows + 1) * PADDED, owned * devices), bf16),
            pltpu.VMEM((owned * devices, side), bf16),
            pltpu.VMEM(((2 * rows + 1) * PADDED, side), bf16),
            pltpu.VMEM((2, groups_x, rows, groups, side), f32),
            pltpu.VMEM((2, groups_x, rows, groups, LANES), f32),
            pltpu.VMEM((2 * half_rows, side), bf16),
            pltpu.VMEM((2 * half_rows, width), bf16),
            pltpu.VMEM((2, groups_x, rows, groups, LANES), f32),
            pltpu.VMEM((half_rows, width), f32),
            pltpu.VMEM((2, groups_x, rows, groups, side), f32),
            pltpu.VMEM((rows, LANES, devices), f32),
        ],
        compiler_params=pltpu.CompilerParams(vmem_limit_bytes=MIDDLE),
        cost_estimate=pl.CostEstimate(
            flops=2**33, bytes_accessed=2**22, transcendentals=0
        ),
        interpret=INTERPRET,
        name="middle",
    )(
        got.reshape(groups_x, groups_z, 2 * step + groups, LANES),
        *tables,
    )
    got = lax.all_to_all(
        sent.reshape(devices, step + groups, LANES), AXES, 0, 0, tiled=True
    )

    high_term, low_response = pl.pallas_call(
        finish_kernel,
        out_shape=(
            jax.ShapeDtypeStruct((groups, LANES, levels), bf16),
            jax.ShapeDtypeStruct((owned, levels), f32),
        ),
        in_specs=[near] * 2,
        out_specs=(anywhere, near),
        scratch_shapes=[
            pltpu.VMEM((LANES * groups, LANES), f32),
            pltpu.VMEM((devices * groups, LANES), f32),
            pltpu.VMEM((levels, LANES), f32),
            pltpu.VMEM((groups, LANES, levels), bf16),
            pltpu.SemaphoreType.DMA((devices * rows // LANES,)),
        ],
        compiler_params=pltpu.CompilerParams(vmem_limit_bytes=FINISH),
        interpret=INTERPRET,
        name="finish",
    )(got, tau_inverse)
    return (high_term.reshape(cells_x, cells_z, levels), low_response)


def solution(mesh):
    placed = (
        P("gx", "gz", None),
        P("gx", "gz", None),
        P(AXES, None),
        P(AXES, None),
        P(AXES),
        P(AXES),
        P(AXES, None, None),
    )
    return jax.shard_map(
        on_device,
        mesh=mesh,
        in_specs=placed,
        out_specs=(P("gx", "gz", None), P(AXES, None)),
        check_vma=False,
    )
```
